128 devices in a mesh: train: 8 (over z, x_hi), serve: 16 (over x_lo, y, core).
Axes of the slice: x: 4 (x_hi: 2, x_lo: 2; x = x_hi * 2 + x_lo), y: 4, z: 4, core: 2. Of those that a mesh axis runs over, the one named last changes fastest.
Arguments:
- train_weights: bfloat16 [16, 7680, 2112], P(None, 'train', 'serve'), may hold values from -6 to 6
- row_offset: int32 [16, 9], replicated, may hold values from 0 to 7168, as said below
- block_group: int32 [16, 224, 1], P(None, 'train'), may hold values from 0 to 15; in each aligned block of 28 rows (0 to 27, 28 to 55, ..., all dimensions but the last counted through in order) at most 3 rows name the same one
Outputs:
- quant_codes: bfloat16 [16, 16, 8, 3, 32, 2112], P(None, 'serve', 'train')
- block_scales: float32 [16, 16, 8, 3, 2112], P(None, 'serve', 'train')
The draws below stay inside these ranges and needn't reach their ends.
Inputs may be any that keep to these rules, and one draw needn't show every extreme that they name: For every layer l: row_offset[l, 0] = 0 and row_offset[l, 8] = 7168; every other row_offset[l, t] lies 1 to 32 rows above or below t * 896, never on it; in every layer one entry lies exactly 32 rows above and another exactly 32 rows below; layer 1 has the opposite sign of layer 0 at every such entry. `block_group`: within each aligned block of 28 entries (one training device's blocks of one layer), no group is named more than 3 times; some group reaches 3 in some of them.
All inputs are finite; a program needn't handle non-finite values.
Results may differ from the reference program's by a relative error of at most 0.001.
Values may be sent and summed in bfloat16 or wider, within the bound.
No kernel may reach another device: no remote copies, remote signals or barrier semaphores. Data moves between devices by JAX's collectives and lax.ppermute only.
A program may use at most 128 MiB of HBM per device.

```python
import math
import jax
import jax.numpy as jnp
import numpy as np
from jax import lax

MODEL_DIM = 7168
LAYERS = 16
BLOCK = 32
SHIFT = 32
FEAT = 2112
ROWS_DEV = 896
SLOT = 960
BLOCKS = 224
BLOCKS_DEV = 28
SLOTS = 3
N_TRAIN = 8
N_SERVE = 16


def draw_train_weights(key, part):
    base_key = jax.random.fold_in(key, 23)
    value_key, quiet_key, scale_key = jax.random.split(base_key, 3)
    full_shape = (LAYERS, N_TRAIN * SLOT, FEAT)
    values = jnp.clip(jax.random.normal(value_key, full_shape, jnp.float32), -6.0, 6.0)
    quiet_mask = jax.random.randint(quiet_key, (LAYERS, MODEL_DIM // BLOCK, FEAT), 0, 8, dtype=jnp.int32) == 0
    buffer_row = jnp.arange(N_TRAIN * SLOT, dtype=jnp.int32)
    owner_dev = buffer_row // SLOT
    global_row = jnp.clip(owner_dev * ROWS_DEV + buffer_row % SLOT - SHIFT, 0, MODEL_DIM - 1).astype(jnp.int32)
    block_of_row = (global_row // BLOCK).astype(jnp.int32)
    quiet_rows = jnp.take(quiet_mask, block_of_row, axis=1)
    damping = jnp.where(quiet_rows, 0.02, 1.0).astype(jnp.float32)
    return (values * damping).astype(jnp.bfloat16)


def draw_row_offset(key, part):
    base_key = jax.random.fold_in(key, 11)
    size_key, sign_key, pick_key = jax.random.split(base_key, 3)
    magnitude = jax.random.randint(size_key, (LAYERS, N_TRAIN - 1), 1, SHIFT + 1, dtype=jnp.int32)
    signs = jax.random.randint(sign_key, (LAYERS, N_TRAIN - 1), 0, 2, dtype=jnp.int32) * 2 - 1
    inner = (magnitude * signs).astype(jnp.int32)
    pick_keys = jax.random.split(pick_key, LAYERS)
    picked = jax.vmap(lambda one_key: jax.random.permutation(one_key, N_TRAIN - 1))(pick_keys)
    column_ids = jnp.arange(N_TRAIN - 1, dtype=jnp.int32)[None, :]
    inner = jnp.where(column_ids == picked[:, 0:1], SHIFT, inner)
    inner = jnp.where(column_ids == picked[:, 1:2], -SHIFT, inner)
    layer_ids = jnp.arange(LAYERS, dtype=jnp.int32)[:, None]
    inner = jnp.where(layer_ids == 1, -inner[0:1], inner).astype(jnp.int32)
    middle = jnp.arange(1, N_TRAIN, dtype=jnp.int32)[None, :] * ROWS_DEV + inner
    start = jnp.zeros((LAYERS, 1), jnp.int32)
    finish = jnp.full((LAYERS, 1), N_TRAIN * ROWS_DEV, jnp.int32)
    return jnp.concatenate([start, middle, finish], axis=1).astype(jnp.int32)


def routed_block(key, own, number, rows, number_of, top, most, slope):
    order = jax.random.permutation(key, number_of)
    crowded, ordinary = shares(number_of, rows * top, most, slope, True), shares(number_of, rows * top, most, slope, False)
    places = jnp.arange(number_of)

    def named(lengths, rotation):
        used = int((lengths > 0).sum())
        fixed = max(1, used // 4)
        moved = fixed + (places - fixed + rotation * (used - fixed)) % max(1, number_of - fixed)
        return jnp.zeros((number_of,), jnp.int32).at[order[jnp.where(places < fixed, places, moved)]].set(jnp.asarray(lengths, jnp.int32))

    lengths = jnp.where(number % 4 == 0, named(crowded, number // 4), named(ordinary, number - number // 4 - 1))
    mixed = jax.random.permutation(jax.random.fold_in(own, 3), number_of)
    donor, sink = mixed[0:number_of // 2 * 2:2], mixed[1:number_of // 2 * 2:2]
    slack = jnp.minimum(lengths[donor] - 1, most - lengths[sink]) // 2
    slack = jnp.where((donor == order[0]) | (sink == order[0]) | (lengths[sink] == 0), 0, jnp.maximum(slack, 0))
    moved = jax.random.randint(jax.random.fold_in(own, 4), (number_of // 2,), 0, 1 << 20) % (slack + 1)
    lengths = lengths.at[donor].add(-moved).at[sink].add(moved)
    labels = jnp.searchsorted(jnp.cumsum(lengths), jnp.arange(rows * top), side="right").astype(jnp.int32)
    listing = labels.reshape(top, rows).T
    listing = listing[jax.random.permutation(jax.random.fold_in(own, 1), rows)]
    rotation = jax.random.randint(jax.random.fold_in(own, 2), (rows, 1), 0, top)
    return jnp.take_along_axis(listing, (jnp.arange(top)[None, :] + rotation) % top, axis=1)


def shares(number_of, total, bound, skew, full):
    portions = [(1 << 20) // math.isqrt(grade ** skew) + 1 for grade in range(1, number_of + 1)]
    largest = bound if full else min(bound, max(-(-total // number_of), total * portions[0] // sum(portions)))
    least = 1 if total - largest >= number_of - 1 else 0
    given, rest = [largest] + [least] * (number_of - 1), total - largest - least * (number_of - 1)
    while rest > 0:
        movable = [i for i in range(1, number_of) if given[i] < largest] or [i for i in range(1, number_of) if given[i] < bound]
        pool, budget = sum([portions[i] for i in movable]), rest
        for i in movable:
            extra = min(bound - given[i], max(1, budget * portions[i] // pool), rest)
            given[i] = given[i] + extra
            rest = rest - extra
    return np.array(given)


def setup_inputs(seed: int = 0) -> dict:
    splits = jax.random.split(jax.random.key(seed), 4)
    train_weights = draw_train_weights(jax.random.fold_in(splits[3], 71), 0)
    row_offset = draw_row_offset(jax.random.fold_in(splits[3], 71), 0)
    block_group_keys = jax.random.split(jax.random.fold_in(splits[2], 1), LAYERS * BLOCKS // BLOCKS_DEV)
    block_group_turns = jax.random.permutation(jax.random.fold_in(splits[2], 3), LAYERS * BLOCKS // BLOCKS_DEV)
    block_group = jax.vmap(lambda own, number: routed_block(jax.random.fold_in(splits[2], 2), own, number, BLOCKS_DEV, N_SERVE, 1, SLOTS, 0))(block_group_keys, block_group_turns).reshape((LAYERS, BLOCKS, 1))
    return {"train_weights": train_weights, "row_offset": row_offset, "block_group": block_group}


def reference(train_weights, row_offset, block_group):
    row_ids = jnp.arange(MODEL_DIM, dtype=jnp.int32)
    block_owner = (jnp.arange(BLOCKS, dtype=jnp.int32) // BLOCKS_DEV).astype(jnp.int32)
    position = jnp.arange(BLOCKS_DEV, dtype=jnp.int32)
    earlier = position[None, :] < position[:, None]

    def one_layer(inputs):
        weights, groups, offsets = inputs
        owner_dev = jnp.sum((row_ids[:, None] >= offsets[None, 1:N_TRAIN]).astype(jnp.int32), axis=1).astype(jnp.int32)
        source = (owner_dev * SLOT + row_ids - owner_dev * ROWS_DEV + SHIFT).astype(jnp.int32)
        gathered = jnp.take(weights, source, axis=0)
        blocks = gathered.reshape(BLOCKS, BLOCK, FEAT).astype(jnp.float32)
        absmax = jnp.max(jnp.abs(blocks), axis=1)
        divisor = jnp.maximum(absmax, 0.25)
        coded = (blocks / divisor[:, None, :]).astype(jnp.bfloat16)
        group_ids = groups[:, 0].astype(jnp.int32)
        per_dev = group_ids.reshape(N_TRAIN, BLOCKS_DEV)
        same_group = per_dev[:, :, None] == per_dev[:, None, :]
        order_in = jnp.sum((same_group & earlier[None]).astype(jnp.int32), axis=2).reshape(BLOCKS).astype(jnp.int32)
        flat_slot = ((group_ids * N_TRAIN + block_owner) * SLOTS + order_in).astype(jnp.int32)
        out_codes = jnp.zeros((N_SERVE * N_TRAIN * SLOTS, BLOCK, FEAT), jnp.bfloat16).at[flat_slot].set(coded)
        out_scales = jnp.zeros((N_SERVE * N_TRAIN * SLOTS, FEAT), jnp.float32).at[flat_slot].set(divisor)
        return (out_codes.reshape(N_SERVE, N_TRAIN, SLOTS, BLOCK, FEAT),
                out_scales.reshape(N_SERVE, N_TRAIN, SLOTS, FEAT))

    quant_codes, block_scales = lax.map(one_layer, (train_weights, block_group, row_offset))
    return quant_codes, block_scales
```

```python
import functools

import jax
import jax.numpy as jnp
from jax import lax
from jax.experimental import pallas as pl
from jax.experimental.pallas import tpu as pltpu
from jax.sharding import PartitionSpec as P

BLOCK = 32
SHIFT = 32
LANES = 128
PACK = 16
NT = (((1,), (1,)), ((), ()))
F32 = jnp.float32
BF16 = jnp.bfloat16
MIB = 1024 * 1024


def iota(shape, dim):
    return lax.broadcasted_iota(jnp.int32, shape, dim)


def identity(n):
    return (iota((n, n), 0) == iota((n, n), 1)).astype(BF16)


def layer_major():
    out, src = iota((PACK * PACK, PACK * PACK), 0), iota((PACK * PACK, PACK * PACK), 1)
    return ((out // PACK == src % PACK) & (out % PACK == src // PACK)).astype(BF16)


def spread(layer):
    src, lane = iota((4 * PACK, LANES), 0), iota((4 * PACK, LANES), 1)
    return ((src % PACK == layer) & (src // PACK == lane % 4)).astype(BF16)


def dot(a, b):
    return jnp.dot(a, b, preferred_element_type=F32)


def edges_kernel(me_ref, first_ref, last_ref, head_ref, tail_ref, planes):
    rows = 2 * SHIFT
    lane = iota((1, 1, LANES), 2)
    perm = layer_major()
    eye = (iota((rows, LANES), 0) == iota((rows, LANES), 1)).astype(BF16)
    zero = jnp.zeros((), BF16)

    def columns(start, count):
        first, last = first_ref[pl.ds(start, count)], last_ref[pl.ds(start, count)]
        return jnp.where(lane < SHIFT, first, jnp.where(lane < rows, last, zero))

    for i in range(LANES // PACK):
        x = columns(PACK * i, PACK).reshape(PACK * PACK, LANES)
        planes[:, PACK * i : PACK * (i + 1), :] = dot(perm, x).astype(BF16).reshape(PACK, PACK, LANES)
    shift = 4 * me_ref[0]
    for layer in range(PACK):
        turned = lax.dot_general(eye, planes[layer], NT, preferred_element_type=F32)
        turned = pltpu.roll(turned, shift, 1).astype(BF16)
        head_ref[layer], tail_ref[layer] = turned[:SHIFT], turned[SHIFT:]
    rest = columns(LANES, 4).reshape(4 * PACK, LANES)
    rest = jnp.concatenate([rest, jnp.zeros_like(rest)], axis=0)
    turned = lax.dot_general(eye, rest, NT, preferred_element_type=F32).astype(BF16)
    head_ref[PACK], tail_ref[PACK] = turned[:SHIFT], turned[SHIFT:]


def turn_kernel(me_ref, x_hbm, rows_ref, rest_ref, x_ref, planes, sems):
    length = x_ref.shape[2]
    steps = LANES // PACK
    parts = [pl.ds(PACK * i, PACK) for i in range(steps)] + [pl.ds(LANES, 4)]
    copies = [pltpu.make_async_copy(x_hbm.at[p], x_ref.at[p], sems.at[i]) for i, p in enumerate(parts)]
    for copy in copies:
        copy.start()
    perm = layer_major()
    for i in range(steps):
        copies[i].wait()
        x = x_ref[parts[i]].reshape(PACK * PACK, length)
        planes[:, PACK * i : PACK * (i + 1), :] = dot(perm, x).astype(BF16).reshape(PACK, PACK, length)
    copies[steps].wait()
    rest = x_ref[parts[steps]].reshape(4 * PACK, length)
    cuts = [(start, min(256, length - start)) for start in range(0, length, 256)]
    for start, size in cuts:
        rest_ref[start : start + size, :] = lax.dot_general(
            identity(size), rest[:, start : start + size], NT, preferred_element_type=F32
        ).astype(BF16)
    shift = 4 * me_ref[0]

    def layer_step(layer, carry):
        for start, size in cuts:
            turned = lax.dot_general(
                identity(size), planes[layer, :, start : start + size], NT, preferred_element_type=F32
            )
            rows_ref[layer, start : start + size, :] = pltpu.roll(turned, shift, 1).astype(BF16)
        return carry

    lax.fori_loop(0, PACK, layer_step, 0)


def pack_kernel(
    slots, me_ref, first_ref, next_ref, group_ref, rows_ref, rest_ref, left_ref, right_ref, out_ref, extra, count
):
    layers, blocks = group_ref.shape
    length = rest_ref.shape[0]
    row = iota((BLOCK, LANES), 0)
    lane_group = iota((BLOCK, LANES), 1) // 4
    me = me_ref[0]
    for g in range(out_ref.shape[0]):
        count[g] = 0

    def layer_step(layer, carry):
        repeat = spread(layer)
        extra[:length] = dot(rest_ref[...], repeat).astype(BF16)
        first, after = first_ref[layer], next_ref[layer] - (blocks - 1) * BLOCK
        left_rest = dot(left_ref[layers][:, : 4 * PACK], repeat).astype(BF16)
        right_rest = dot(right_ref[layers][:, : 4 * PACK], repeat).astype(BF16)
        for b in range(blocks):
            at = SHIFT + BLOCK * b
            block = rows_ref[layer, at : at + BLOCK, :]
            rest = extra[at : at + BLOCK, :]
            if b == 0:
                block = jnp.where(row < first, left_ref[layer], block)
                rest = jnp.where(row < first, left_rest, rest)
            if b == blocks - 1:
                block = jnp.where(row >= after, right_ref[layer], block)
                rest = jnp.where(row >= after, right_rest, rest)
            group = group_ref[layer, b]
            j = count[group]
            count[group] = j + 1
            out_ref[group, j] = block
            tile = slots + lax.shift_right_logical(j, 5)
            place = (j + me) & 31
            out_ref[group, tile] = jnp.where(lane_group == place, rest, out_ref[group, tile])
        return carry

    lax.fori_loop(0, layers, layer_step, 0)


def join_kernel(slots, base_ref, used_ref, in_hbm, codes_ref, scale_ref, held, sems):
    peers, units = in_hbm.shape[0], in_hbm.shape[1]
    per_layer = codes_ref.shape[1]
    layer = pl.program_id(0)
    cuts = [(slots, units - slots)] + [(start, min(8, slots - start)) for start in range(0, slots, 8)]
    copies = [
        pltpu.make_async_copy(in_hbm.at[:, pl.ds(s, n)], held.at[:, pl.ds(s, n)], sems.at[i])
        for i, (s, n) in enumerate(cuts)
    ]

    @pl.when(layer == 0)
    def _():
        for copy in copies:
            copy.start()
        copies[0].wait()

    for i in range(1, len(copies)):
        @pl.when(layer == cuts[i][0] // per_layer)
        def _(i=i):
            copies[i].wait()

    lane = iota((BLOCK, LANES), 1)
    base, used = base_ref[layer], used_ref[layer]
    width = codes_ref.shape[3]
    for k in range(per_layer):

        @pl.when(k < used)
        def _(k=k):
            j = base + k
            tile = slots + lax.shift_right_logical(j, 5)
            jj = j & 31
            source = (lane // 4 - jj) & 31
            rest = jnp.zeros((BLOCK, LANES), F32)
            for s in range(peers):
                rest = jnp.where(source == s, held[s, tile].astype(F32), rest)
            rest = pltpu.roll(rest, (LANES - 4 * jj) & (LANES - 1), 1)
            before = None
            for t in range(peers + 1):
                x = rest
                if before is not None:
                    x = jnp.where(lane < 4 * t - 4, before, x)
                if t < peers:
                    own = held[t, j].astype(F32)
                    x = own if t == 0 else jnp.where(lane >= 4 * t, own, x)
                    before = own
                size = min(LANES, width - LANES * t)
                top = jnp.maximum(jnp.max(jnp.abs(x), axis=0, keepdims=True), 0.25)
                scale_ref[k, :, LANES * t : LANES * t + size] = top[:, :size]
                code = (x * (1.0 / top)).astype(BF16)
                codes_ref[0, k, :, LANES * t : LANES * t + size] = code[:, :size]

        @pl.when(k >= used)
        def _(k=k):
            codes_ref[0, k] = jnp.zeros((BLOCK, width), BF16)
            scale_ref[k] = jnp.zeros((1, width), F32)


def in_vmem():
    return pl.BlockSpec(memory_space=pltpu.VMEM)


def in_smem():
    return pl.BlockSpec(memory_space=pltpu.SMEM)


def shards(train_weights, row_offset, block_group):
    train_n = lax.axis_size("train")
    serve_n = lax.axis_size("serve")
    train_idx = lax.axis_index("train")
    serve_idx = lax.axis_index("serve").astype(jnp.int32)
    layers, buffer_len, columns = train_weights.shape
    rows_dev = buffer_len - 2 * SHIFT
    blocks_dev = block_group.shape[1]
    per_layer = (blocks_dev + serve_n - 1) // serve_n + 1
    slots = layers * per_layer
    units = slots + -(-slots // 32)
    width = columns * serve_n
    groups = block_group[:, :, 0]
    me = serve_idx.reshape(1)
    by_column = jnp.transpose(train_weights, (2, 0, 1))

    tile = (columns, layers, LANES)
    edge = jax.ShapeDtypeStruct((layers + 1, SHIFT, LANES), BF16)
    head, tail = pl.pallas_call(
        edges_kernel,
        grid=(1,),
        in_specs=[
            in_smem(),
            pl.BlockSpec(tile, lambda i: (0, 0, 0)),
            pl.BlockSpec(tile, lambda i: (0, 0, (buffer_len - 2 * SHIFT) // LANES)),
        ],
        out_specs=[in_vmem(), in_vmem()],
        out_shape=[edge, edge],
        scratch_shapes=[pltpu.VMEM((layers, LANES, LANES), BF16)],
        compiler_params=pltpu.CompilerParams(vmem_limit_bytes=16 * MIB),
        cost_estimate=pl.CostEstimate(flops=10**8, bytes_accessed=10**6, transcendentals=0),
        name="edges",
    )(me, by_column, by_column)
    left = lax.ppermute(tail, "train", [(i, i + 1) for i in range(train_n - 1)])
    right = lax.ppermute(head, "train", [(i + 1, i) for i in range(train_n - 1)])

    rows, rest = pl.pallas_call(
        turn_kernel,
        in_specs=[in_smem(), pl.BlockSpec(memory_space=pl.ANY)],
        out_specs=[in_vmem(), in_vmem()],
        out_shape=[
            jax.ShapeDtypeStruct((layers, buffer_len, LANES), BF16),
            jax.ShapeDtypeStruct((buffer_len, 4 * PACK), BF16),
        ],
        scratch_shapes=[
            pltpu.VMEM((columns, layers, buffer_len), BF16),
            pltpu.VMEM((layers, LANES, buffer_len), BF16),
            pltpu.SemaphoreType.DMA((LANES // PACK + 1,)),
        ],
        compiler_params=pltpu.CompilerParams(vmem_limit_bytes=32 * MIB),
        cost_estimate=pl.CostEstimate(flops=3 * 10**9, bytes_accessed=9 * 10**6, transcendentals=0),
        name="turn",
    )(me, by_column)

    entries = jnp.arange(train_n + 1, dtype=jnp.int32)
    first_row = jnp.sum(jnp.where(entries[None, :] == train_idx, row_offset, 0), axis=1) - train_idx * rows_dev
    next_row = jnp.sum(jnp.where(entries[None, :] == train_idx + 1, row_offset, 0), axis=1) - train_idx * rows_dev
    sent = pl.pallas_call(
        functools.partial(pack_kernel, slots),
        in_specs=[in_smem()] * 4 + [in_vmem()] * 4,
        out_specs=in_vmem(),
        out_shape=jax.ShapeDtypeStruct((serve_n, units, BLOCK, LANES), BF16),
        scratch_shapes=[pltpu.VMEM((buffer_len, LANES), BF16), pltpu.SMEM((serve_n,), jnp.int32)],
        compiler_params=pltpu.CompilerParams(vmem_limit_bytes=24 * MIB),
        cost_estimate=pl.CostEstimate(flops=10**9, bytes_accessed=10**7, transcendentals=0),
        name="pack",
    )(me, first_row, next_row, groups, rows, rest, left, right)

    got = lax.all_to_all(sent, "serve", split_axis=0, concat_axis=0, tiled=True)

    used = jnp.sum((groups == serve_idx).astype(jnp.int32), axis=1)
    order = jnp.arange(layers, dtype=jnp.int32)
    base = jnp.sum(jnp.where(order[None, :] < order[:, None], used[None, :], 0), axis=1)
    codes, scales = pl.pallas_call(
        functools.partial(join_kernel, slots),
        grid=(layers,),
        in_specs=[in_smem(), in_smem(), pl.BlockSpec(memory_space=pl.ANY)],
        out_specs=[
            pl.BlockSpec((1, per_layer, BLOCK, width), lambda i: (i, 0, 0, 0)),
            pl.BlockSpec((per_layer, 1, width), lambda i: (i, 0, 0)),
        ],
        out_shape=[
            jax.ShapeDtypeStruct((layers, per_layer, BLOCK, width), BF16),
            jax.ShapeDtypeStruct((layers * per_layer, 1, width), F32),
        ],
        scratch_shapes=[
            pltpu.VMEM((serve_n, units, BLOCK, LANES), BF16),
            pltpu.SemaphoreType.DMA((1 + -(-slots // 8),)),
        ],
        compiler_params=pltpu.CompilerParams(
            dimension_semantics=("arbitrary",), vmem_limit_bytes=24 * MIB
        ),
        cost_estimate=pl.CostEstimate(flops=10**8, bytes_accessed=13 * 10**6, transcendentals=0),
        name="join",
    )(base, used, got)
    return (
        codes.reshape(layers, 1, 1, per_layer, BLOCK, width),
        scales.reshape(layers, 1, 1, per_layer, width),
    )


def solution(mesh):
    return jax.shard_map(
        shards,
        mesh=mesh,
        in_specs=(P(None, "train", "serve"), P(), P(None, "train", None)),
        out_specs=(P(None, "serve", "train", None, None, None), P(None, "serve", "train", None, None)),
        check_vma=False,
    )
```

```python
import functools

import jax
import jax.numpy as jnp
from jax import lax
from jax.experimental import pallas as pl
from jax.experimental.pallas import tpu as pltpu
from jax.sharding import Mesh
from jax.sharding import PartitionSpec as P

BLOCK = 32
SHIFT = 32
LANES = 128
PACK = 16
NT = (((1,), (1,)), ((), ()))
F32 = jnp.float32
BF16 = jnp.bfloat16
CORES = 2
SERVE = ("chip", "core")
MIB = 1024 * 1024


def iota(shape, dim):
    return lax.broadcasted_iota(jnp.int32, shape, dim)


def identity(n):
    return (iota((n, n), 0) == iota((n, n), 1)).astype(BF16)


def layer_major():
    out, src = iota((PACK * PACK, PACK * PACK), 0), iota((PACK * PACK, PACK * PACK), 1)
    return ((out // PACK == src % PACK) & (out % PACK == src // PACK)).astype(BF16)


def spread(layer):
    src, lane = iota((4 * PACK, LANES), 0), iota((4 * PACK, LANES), 1)
    return ((src % PACK == layer) & (src // PACK == lane % 4)).astype(BF16)


def dot(a, b):
    return jnp.dot(a, b, preferred_element_type=F32)


def edges_kernel(me_ref, first_ref, last_ref, head_ref, tail_ref, planes):
    rows = 2 * SHIFT
    lane = iota((1, 1, LANES), 2)
    perm = layer_major()
    eye = (iota((rows, LANES), 0) == iota((rows, LANES), 1)).astype(BF16)
    zero = jnp.zeros((), BF16)

    def columns(start, count):
        first, last = first_ref[pl.ds(start, count)], last_ref[pl.ds(start, count)]
        return jnp.where(lane < SHIFT, first, jnp.where(lane < rows, last, zero))

    for i in range(LANES // PACK):
        x = columns(PACK * i, PACK).reshape(PACK * PACK, LANES)
        planes[:, PACK * i : PACK * (i + 1), :] = dot(perm, x).astype(BF16).reshape(PACK, PACK, LANES)
    shift = 4 * me_ref[0]
    for layer in range(PACK):
        turned = lax.dot_general(eye, planes[layer], NT, preferred_element_type=F32)
        turned = pltpu.roll(turned, shift, 1).astype(BF16)
        head_ref[layer], tail_ref[layer] = turned[:SHIFT], turned[SHIFT:]
    rest = columns(LANES, 4).reshape(4 * PACK, LANES)
    rest = jnp.concatenate([rest, jnp.zeros_like(rest)], axis=0)
    turned = lax.dot_general(eye, rest, NT, preferred_element_type=F32).astype(BF16)
    head_ref[PACK], tail_ref[PACK] = turned[:SHIFT], turned[SHIFT:]


def turn_kernel(me_ref, x_hbm, rows_hbm, rest_ref, x_ref, planes, rows_ref, sems, out_sem):
    length = x_ref.shape[2]
    steps = LANES // PACK
    parts = [pl.ds(PACK * i, PACK) for i in range(steps)] + [pl.ds(LANES, 4)]
    copies = [pltpu.make_async_copy(x_hbm.at[p], x_ref.at[p], sems.at[i]) for i, p in enumerate(parts)]
    for copy in copies:
        copy.start()
    perm = layer_major()
    for i in range(steps):
        copies[i].wait()
        x = x_ref[parts[i]].reshape(PACK * PACK, length)
        planes[:, PACK * i : PACK * (i + 1), :] = dot(perm, x).astype(BF16).reshape(PACK, PACK, length)
    copies[steps].wait()
    rest = x_ref[parts[steps]].reshape(4 * PACK, length)
    cuts = [(start, min(256, length - start)) for start in range(0, length, 256)]
    for start, size in cuts:
        rest_ref[start : start + size, :] = lax.dot_general(
            identity(size), rest[:, start : start + size], NT, preferred_element_type=F32
        ).astype(BF16)
    shift = 4 * me_ref[0]

    def layer_step(layer, carry):
        for start, size in cuts:
            turned = lax.dot_general(
                identity(size), planes[layer, :, start : start + size], NT, preferred_element_type=F32
            )
            rows_ref[layer, start : start + size, :] = pltpu.roll(turned, shift, 1).astype(BF16)
        pltpu.make_async_copy(rows_ref.at[layer], rows_hbm.at[layer], out_sem).start()
        return carry

    lax.fori_loop(0, PACK, layer_step, 0)
    pltpu.make_async_copy(rows_ref, rows_hbm, out_sem).wait()


def pack_kernel(
    slots,
    me_ref,
    first_ref,
    next_ref,
    group_ref,
    rows_hbm,
    rest_ref,
    left_ref,
    right_ref,
    own_hbm,
    other_hbm,
    rows_ref,
    out_ref,
    extra,
    count,
    sems,
    out_sems,
):
    layers, blocks = group_ref.shape
    peers = out_ref.shape[0] // CORES
    loads = [pltpu.make_async_copy(rows_hbm.at[i], rows_ref.at[i], sems.at[i]) for i in range(layers)]
    for load in loads:
        load.start()
    length = rest_ref.shape[0]
    row = iota((BLOCK, LANES), 0)
    lane_group = iota((BLOCK, LANES), 1) // 4
    me = me_ref[0]
    core = me & 1
    for g in range(out_ref.shape[0]):
        count[g] = 0

    def layer_step(layer, carry):
        pltpu.make_async_copy(rows_hbm.at[layer], rows_ref.at[layer], sems.at[layer]).wait()
        repeat = spread(layer)
        extra[:length] = dot(rest_ref[...], repeat).astype(BF16)
        first, after = first_ref[layer], next_ref[layer] - (blocks - 1) * BLOCK
        left_rest = dot(left_ref[layers][:, : 4 * PACK], repeat).astype(BF16)
        right_rest = dot(right_ref[layers][:, : 4 * PACK], repeat).astype(BF16)
        for b in range(blocks):
            at = SHIFT + BLOCK * b
            block = rows_ref[layer, at : at + BLOCK, :]
            rest = extra[at : at + BLOCK, :]
            if b == 0:
                block = jnp.where(row < first, left_ref[layer], block)
                rest = jnp.where(row < first, left_rest, rest)
            if b == blocks - 1:
                block = jnp.where(row >= after, right_ref[layer], block)
                rest = jnp.where(row >= after, right_rest, rest)
            group = group_ref[layer, b]
            j = count[group]
            count[group] = j + 1
            place = ((group & 1) ^ core) * peers + lax.shift_right_logical(group, 1)
            out_ref[place, j] = block
            tile = slots + lax.shift_right_logical(j, 5)
            out_ref[place, tile] = jnp.where(lane_group == ((j + me) & 31), rest, out_ref[place, tile])
        return carry

    lax.fori_loop(0, layers, layer_step, 0)
    stores = [
        pltpu.make_async_copy(out_ref.at[pl.ds(peers * i, peers)], ref, out_sems.at[i])
        for i, ref in enumerate((own_hbm, other_hbm))
    ]
    for store in stores:
        store.start()
    for store in stores:
        store.wait()


def join_kernel(slots, me_ref, base_ref, used_ref, own_hbm, other_hbm, codes_ref, scale_ref, held, sems):
    peers, units = CORES * own_hbm.shape[0], own_hbm.shape[1]
    core = me_ref[0] & 1
    per_layer = codes_ref.shape[1]
    layer = pl.program_id(0)
    cuts = [(slots, units - slots)] + [(start, min(8, slots - start)) for start in range(0, slots, 8)]
    copies = [
        [
            pltpu.make_async_copy(ref.at[:, pl.ds(s, n)], held.at[place, :, pl.ds(s, n)], sems.at[2 * i + h])
            for h, (ref, place) in enumerate(((own_hbm, core), (other_hbm, 1 - core)))
        ]
        for i, (s, n) in enumerate(cuts)
    ]

    @pl.when(layer == 0)
    def _():
        for pair in copies:
            for copy in pair:
                copy.start()
        for copy in copies[0]:
            copy.wait()

    for i in range(1, len(copies)):
        @pl.when(layer == cuts[i][0] // per_layer)
        def _(i=i):
            for copy in copies[i]:
                copy.wait()

    lane = iota((BLOCK, LANES), 1)
    base, used = base_ref[layer], used_ref[layer]
    width = codes_ref.shape[3]
    for k in range(per_layer):

        @pl.when(k < used)
        def _(k=k):
            j = base + k
            tile = slots + lax.shift_right_logical(j, 5)
            jj = j & 31
            source = (lane // 4 - jj) & 31
            rest = jnp.zeros((BLOCK, LANES), F32)
            for s in range(peers):
                rest = jnp.where(source == s, held[s % CORES, s // CORES, tile].astype(F32), rest)
            rest = pltpu.roll(rest, (LANES - 4 * jj) & (LANES - 1), 1)
            before = None
            for t in range(peers + 1):
                x = rest
                if before is not None:
                    x = jnp.where(lane < 4 * t - 4, before, x)
                if t < peers:
                    own = held[t % CORES, t // CORES, j].astype(F32)
                    x = own if t == 0 else jnp.where(lane >= 4 * t, own, x)
                    before = own
                size = min(LANES, width - LANES * t)
                top = jnp.maximum(jnp.max(jnp.abs(x), axis=0, keepdims=True), 0.25)
                scale_ref[k, :, LANES * t : LANES * t + size] = top[:, :size]
                code = (x * (1.0 / top)).astype(BF16)
                codes_ref[0, k, :, LANES * t : LANES * t + size] = code[:, :size]

        @pl.when(k >= used)
        def _(k=k):
            codes_ref[0, k] = jnp.zeros((BLOCK, width), BF16)
            scale_ref[k] = jnp.zeros((1, width), F32)


def in_vmem():
    return pl.BlockSpec(memory_space=pltpu.VMEM)


def in_hbm():
    return pl.BlockSpec(memory_space=pltpu.HBM)


def hbm(value):
    return pltpu.with_memory_space_constraint(value, pltpu.HBM)


def in_smem():
    return pl.BlockSpec(memory_space=pltpu.SMEM)


def shards(train_weights, row_offset, block_group):
    train_n = lax.axis_size("train")
    serve_n = lax.axis_size(SERVE)
    train_idx = lax.axis_index("train")
    serve_idx = lax.axis_index(SERVE).astype(jnp.int32)
    layers, buffer_len, columns = train_weights.shape
    rows_dev = buffer_len - 2 * SHIFT
    blocks_dev = block_group.shape[1]
    per_layer = (blocks_dev + serve_n - 1) // serve_n + 1
    slots = layers * per_layer
    units = slots + -(-slots // 32)
    width = columns * serve_n
    groups = block_group[:, :, 0]
    me = serve_idx.reshape(1)
    by_column = hbm(jnp.transpose(train_weights, (2, 0, 1)))

    tile = (columns, layers, LANES)
    edge = jax.ShapeDtypeStruct((layers + 1, SHIFT, LANES), BF16)
    head, tail = pl.pallas_call(
        edges_kernel,
        grid=(1,),
        in_specs=[
            in_smem(),
            pl.BlockSpec(tile, lambda i: (0, 0, 0)),
            pl.BlockSpec(tile, lambda i: (0, 0, (buffer_len - 2 * SHIFT) // LANES)),
        ],
        out_specs=[in_vmem(), in_vmem()],
        out_shape=[edge, edge],
        scratch_shapes=[pltpu.VMEM((layers, LANES, LANES), BF16)],
        compiler_params=pltpu.CompilerParams(vmem_limit_bytes=8 * MIB),
        cost_estimate=pl.CostEstimate(flops=10**8, bytes_accessed=10**6, transcendentals=0),
        name="edges",
    )(me, by_column, by_column)
    left = lax.ppermute(tail, "train", [(i, i + 1) for i in range(train_n - 1)])
    right = lax.ppermute(head, "train", [(i + 1, i) for i in range(train_n - 1)])

    rows, rest = pl.pallas_call(
        turn_kernel,
        in_specs=[in_smem(), in_hbm()],
        out_specs=[in_hbm(), in_vmem()],
        out_shape=[
            pltpu.HBM((layers, buffer_len, LANES), BF16),
            jax.ShapeDtypeStruct((buffer_len, 4 * PACK), BF16),
        ],
        scratch_shapes=[
            pltpu.VMEM((columns, layers, buffer_len), BF16),
            pltpu.VMEM((layers, LANES, buffer_len), BF16),
            pltpu.VMEM((layers, buffer_len, LANES), BF16),
            pltpu.SemaphoreType.DMA((LANES // PACK + 1,)),
            pltpu.SemaphoreType.DMA,
        ],
        compiler_params=pltpu.CompilerParams(vmem_limit_bytes=24 * MIB),
        cost_estimate=pl.CostEstimate(flops=3 * 10**9, bytes_accessed=9 * 10**6, transcendentals=0),
        name="turn",
    )(me, by_column)

    entries = jnp.arange(train_n + 1, dtype=jnp.int32)
    first_row = jnp.sum(jnp.where(entries[None, :] == train_idx, row_offset, 0), axis=1) - train_idx * rows_dev
    next_row = jnp.sum(jnp.where(entries[None, :] == train_idx + 1, row_offset, 0), axis=1) - train_idx * rows_dev
    half = pltpu.HBM((serve_n // CORES, units, BLOCK, LANES), BF16)
    own, other = pl.pallas_call(
        functools.partial(pack_kernel, slots),
        in_specs=[in_smem()] * 4 + [in_hbm()] + [in_vmem()] * 3,
        out_specs=[in_hbm()] * CORES,
        out_shape=[half] * CORES,
        scratch_shapes=[
            pltpu.VMEM((layers, buffer_len, LANES), BF16),
            pltpu.VMEM((serve_n, units, BLOCK, LANES), BF16),
            pltpu.VMEM((buffer_len, LANES), BF16),
            pltpu.SMEM((serve_n,), jnp.int32),
            pltpu.SemaphoreType.DMA((layers,)),
            pltpu.SemaphoreType.DMA((CORES,)),
        ],
        compiler_params=pltpu.CompilerParams(vmem_limit_bytes=24 * MIB),
        cost_estimate=pl.CostEstimate(flops=10**9, bytes_accessed=10**7, transcendentals=0),
        name="pack",
    )(me, first_row, next_row, groups, hbm(rows), rest, left, right)

    from_own = lax.all_to_all(own, "chip", split_axis=0, concat_axis=0, tiled=True)
    passed = lax.ppermute(other, "core", [(0, 1), (1, 0)])
    from_other = lax.all_to_all(passed, "chip", split_axis=0, concat_axis=0, tiled=True)

    used = jnp.sum((groups == serve_idx).astype(jnp.int32), axis=1)
    order = jnp.arange(layers, dtype=jnp.int32)
    base = jnp.sum(jnp.where(order[None, :] < order[:, None], used[None, :], 0), axis=1)
    codes, scales = pl.pallas_call(
        functools.partial(join_kernel, slots),
        grid=(layers,),
        in_specs=[in_smem()] * 3 + [in_hbm()] * CORES,
        out_specs=[
            pl.BlockSpec((1, per_layer, BLOCK, width), lambda i: (i, 0, 0, 0)),
            pl.BlockSpec((per_layer, 1, width), lambda i: (i, 0, 0)),
        ],
        out_shape=[
            jax.ShapeDtypeStruct((layers, per_layer, BLOCK, width), BF16),
            jax.ShapeDtypeStruct((layers * per_layer, 1, width), F32),
        ],
        scratch_shapes=[
            pltpu.VMEM((CORES, serve_n // CORES, units, BLOCK, LANES), BF16),
            pltpu.SemaphoreType.DMA((CORES * (1 + -(-slots // 8)),)),
        ],
        compiler_params=pltpu.CompilerParams(
            dimension_semantics=("arbitrary",), vmem_limit_bytes=24 * MIB
        ),
        cost_estimate=pl.CostEstimate(flops=10**8, bytes_accessed=13 * 10**6, transcendentals=0),
        name="join",
    )(me, base, used, hbm(from_own), hbm(from_other))
    return (
        codes.reshape(layers, 1, 1, per_layer, BLOCK, width),
        scales.reshape(layers, 1, 1, per_layer, width),
    )


def solution(mesh):
    cores = Mesh(
        mesh.devices.reshape(mesh.shape["train"], mesh.shape["serve"] // CORES, CORES),
        ("train", *SERVE),
    )
    return jax.shard_map(
        shards,
        mesh=cores,
        in_specs=(P(None, "train", SERVE), P(), P(None, "train", None)),
        out_specs=(P(None, SERVE, "train", None, None, None), P(None, SERVE, "train", None, None)),
        check_vma=False,
    )
```

```python
import functools

import jax
import jax.numpy as jnp
from jax import lax
from jax.experimental import pallas as pl
from jax.experimental.pallas import tpu as pltpu
from jax.sharding import Mesh
from jax.sharding import PartitionSpec as P


BLOCK = 32
SHIFT = 32
LANES = 128
PACK = 16
SERVE = ("x", "y", "core")
SIDES = (2, 4, 2)
OFFSETS = [(dx, dy, dc) for dx, dy in ((1, 2), (1, 1), (1, 3), (0, 2), (1, 0), (0, 1), (0, 3), (0, 0)) for dc in (1, 0)]
FIRST = 32
EACH = 8
NT = (((1,), (1,)), ((), ()))
F32 = jnp.float32
BF16 = jnp.bfloat16
MIB = 1024 * 1024


def iota(shape, dim):
    return lax.broadcasted_iota(jnp.int32, shape, dim)


def identity(n):
    return (iota((n, n), 0) == iota((n, n), 1)).astype(BF16)


def layer_major():
    out, src = iota((PACK * PACK, PACK * PACK), 0), iota((PACK * PACK, PACK * PACK), 1)
    return ((out // PACK == src % PACK) & (out % PACK == src // PACK)).astype(BF16)


def rest_major():
    out, src = iota((LANES, 4 * PACK), 0), iota((LANES, 4 * PACK), 1)
    return ((out // 4 == src % PACK) & (out % 4 == src // PACK)).astype(BF16)


def dot(a, b):
    return jnp.dot(a, b, preferred_element_type=F32)


def turn(eye, value):
    return lax.dot_general(eye, value, NT, preferred_element_type=F32)


def ahead(me, offset):
    dx, dy, dc = offset
    return (me ^ (8 * dx + dc)) & 9 | ((me >> 1) + dy & 3) << 1


def behind(me, offset):
    dx, dy, dc = offset
    return ahead(me, (dx, -dy & 3, dc))


def edges_kernel(me_ref, first_ref, last_ref, head_ref, tail_ref, planes):
    rows = 2 * SHIFT
    lane = iota((1, 1, LANES), 2)
    perm = layer_major()
    eye = (iota((rows, LANES), 0) == iota((rows, LANES), 1)).astype(BF16)
    zero = jnp.zeros((), BF16)

    def columns(start, count):
        first, last = first_ref[pl.ds(start, count)], last_ref[pl.ds(start, count)]
        return jnp.where(lane < SHIFT, first, jnp.where(lane < rows, last, zero)).reshape(count * PACK, LANES)

    for i in range(LANES // PACK):
        x = columns(PACK * i, PACK)
        planes[:, PACK * i : PACK * (i + 1), :] = dot(perm, x).astype(BF16).reshape(PACK, PACK, LANES)
    shift = 4 * me_ref[0]
    for layer in range(PACK):
        turned = pltpu.roll(turn(eye, planes[layer]), shift, 1).astype(BF16)
        head_ref[layer], tail_ref[layer] = turned[:SHIFT], turned[SHIFT:]
    turned = turn(eye, dot(rest_major(), columns(LANES, 4)).astype(BF16)).astype(BF16)
    head_ref[PACK], tail_ref[PACK] = turned[:SHIFT], turned[SHIFT:]


def planes_kernel(slots, me_ref, group_ref, x_hbm, planes_ref, rest_ref, table_ref, count_ref, x_ref, sems):
    length = x_ref.shape[2]
    steps = LANES // PACK
    spare = PACK - 4
    parts = [(LANES - spare, spare, 0)] + [(PACK * i, PACK, spare + PACK * i) for i in range(steps)]
    parts.append((LANES, 4, spare + LANES))
    copies = [
        pltpu.make_async_copy(x_hbm.at[pl.ds(src, n)], x_ref.at[pl.ds(dst, n)], sems.at[i])
        for i, (src, n, dst) in enumerate(parts)
    ]
    for copy in copies:
        copy.start()
    layers, blocks = group_ref.shape
    for g in range(count_ref.shape[0]):
        count_ref[g] = 0
    perm = layer_major()
    turns, part = me_ref[0] >> 2, 4 * (me_ref[0] & 3)
    copies[0].wait()
    for i in range(steps):
        copies[i + 1].wait()
        x = x_ref[pl.ds(spare + PACK * i - part, PACK)].reshape(PACK * PACK, length)
        at = pl.multiple_of(PACK * ((i + turns) & (steps - 1)), PACK)
        planes_ref[:, pl.ds(at, PACK), :] = dot(perm, x).astype(BF16).reshape(PACK, PACK, length)
        for layer in range(layers * i // steps, layers * (i + 1) // steps):
            for b in range(blocks):
                group = group_ref[layer, b]
                j = count_ref[group]
                count_ref[group] = j + 1
                table_ref[group * slots + j] = (layer << 10) + SHIFT + BLOCK * b
    copies[steps + 1].wait()
    rest = dot(rest_major(), x_ref[pl.ds(spare + LANES, 4)].reshape(4 * PACK, length)).astype(BF16)
    for start in range(0, length, 256):
        size = min(256, length - start)
        rest_ref[start : start + size, :] = turn(identity(size), rest[:, start : start + size])


def pack_kernel(
    slots, me_ref, first_ref, next_ref, table_ref, count_ref, planes_ref, rest_ref, left_ref, right_ref, *refs
):
    peers = len(OFFSETS)
    sets, third_ref, (rows_ref, extra_ref) = (refs[:peers], refs[peers : 2 * peers]), refs[2 * peers], refs[2 * peers + 1 :]
    layers, _, length = planes_ref.shape
    row = iota((BLOCK, LANES), 0)
    lane_group = iota((BLOCK, LANES), 1) >> 2
    me = me_ref[0]
    last = length - 2 * SHIFT

    def pair_step(pair, carry):
        both = planes_ref[pl.ds(2 * pair, 2)].reshape(2 * LANES, length)
        for start in range(0, length, 256):
            size = min(256, length - start)
            turned = turn(identity(size), both[:, start : start + size]).astype(BF16)
            rows_ref[2 * pair, start : start + size, :] = turned[:, :LANES]
            rows_ref[2 * pair + 1, start : start + size, :] = turned[:, LANES:]
        return carry

    lax.fori_loop(0, layers // 2, pair_step, 0)

    def edge_step(layer, carry):
        first, after = carry
        start, end = first_ref[layer], next_ref[layer] - (last - SHIFT)
        rows_ref[layer, SHIFT : 2 * SHIFT] = jnp.where(row < start, left_ref[layer], rows_ref[layer, SHIFT : 2 * SHIFT])
        rows_ref[layer, last : last + SHIFT] = jnp.where(row >= end, right_ref[layer], rows_ref[layer, last : last + SHIFT])
        return jnp.where(lane_group == layer, start, first), jnp.where(lane_group == layer, end, after)

    nothing = jnp.zeros((BLOCK, LANES), jnp.int32)
    first, after = lax.fori_loop(0, layers, edge_step, (nothing, nothing), unroll=4)
    extra_ref[...] = rest_ref[...]
    extra_ref[SHIFT : 2 * SHIFT] = jnp.where(row < first, left_ref[layers].astype(F32), rest_ref[SHIFT : 2 * SHIFT])
    extra_ref[last : last + SHIFT] = jnp.where(row >= after, right_ref[layers].astype(F32), rest_ref[last : last + SHIFT])

    def fill(ref, group, start, size):
        used = count_ref[group]

        def step(i, rest):
            for u in range(4):
                n = 4 * i + u
                j = start + n
                entry = jnp.where(j < used, table_ref[group * slots + j], SHIFT)
                layer, at = entry >> 10, pl.multiple_of(entry & 1023, BLOCK)
                ref[n] = rows_ref[layer, pl.ds(at, BLOCK), :]
                place = j + me & 31
                moved = pltpu.roll(extra_ref[pl.ds(at, BLOCK), :], 4 * (place - layer) & (LANES - 1), 1)
                rest = jnp.where(lane_group == place, moved, rest)
            return rest

        ref[size] = lax.fori_loop(0, size // 4, step, jnp.zeros((BLOCK, LANES), F32)).astype(BF16)

    for p, offset in enumerate(OFFSETS):
        group = ahead(me, offset)
        fill(sets[0][p], group, 0, FIRST)
        fill(sets[1][p], group, FIRST, EACH)

        @pl.when(count_ref[group] > FIRST + EACH)
        def _(group=group):
            fill(third_ref.at[group], group, FIRST + EACH, EACH)


def join_slot(held, n, tile, jj, code_ref, scale_ref, width):
    peers = held.shape[0]
    lane = iota((BLOCK, LANES), 1)
    source = (lane >> 2) - jj & 31
    rest = jnp.zeros((BLOCK, LANES), F32)
    for s in range(peers):
        rest = jnp.where(source == s, held[s, tile].astype(F32), rest)
    rest = pltpu.roll(rest, -4 * jj & (LANES - 1), 1)
    before = None
    for t in range(peers + 1):
        x = rest
        if before is not None:
            x = jnp.where(lane < 4 * t - 4, before, x)
        if t < peers:
            own = held[t, n].astype(F32)
            x = own if t == 0 else jnp.where(lane >= 4 * t, own, x)
            before = own
        size = min(LANES, width - LANES * t)
        top = jnp.maximum(jnp.max(jnp.abs(x), axis=0, keepdims=True), 0.25)
        scale_ref[:, LANES * t : LANES * t + size] = top[:, :size]
        code_ref[:, LANES * t : LANES * t + size] = (x * (1.0 / top)).astype(BF16)[:, :size]


def write_slots(base_ref, used_ref, codes_hbm, scale_hbm, code_ref, scale_ref, code_sem, scale_sem, low, high, compute):
    layers = base_ref.shape[0]
    per_layer = codes_hbm.shape[0] // layers
    ring = code_ref.shape[0]

    def stores(i, slot):
        return (
            pltpu.make_async_copy(code_ref.at[i], codes_hbm.at[slot], code_sem.at[i]),
            pltpu.make_async_copy(scale_ref.at[i], scale_hbm.at[slot], scale_sem.at[i]),
        )

    def layer_step(layer, done):
        for k in range(per_layer):
            j = base_ref[layer] + k
            mine = (k < used_ref[layer]) & (j >= low) & (j < high)
            i = done & (ring - 1)

            @pl.when(mine)
            def _(j=j, i=i, done=done, k=k):
                @pl.when(done >= ring)
                def _():
                    for store in stores(i, 0):
                        store.wait()

                compute(j, code_ref.at[i], scale_ref.at[i])
                for store in stores(i, per_layer * layer + k):
                    store.start()

            done = done + mine.astype(jnp.int32)
        return done

    done = lax.fori_loop(0, layers, layer_step, jnp.int32(0))
    for i in range(ring):

        @pl.when(done > i)
        def _(i=i):
            for store in stores(i, 0):
                store.wait()


def join_first_kernel(me_ref, base_ref, used_ref, *refs):
    peers = len(OFFSETS)
    parts, (codes_hbm, scale_hbm) = refs[:peers], refs[peers : peers + 2]
    held, code_ref, scale_ref, zero_code, zero_scale, sems, code_sem, scale_sem, zero_sem = refs[peers + 2 :]
    me, width = me_ref[0], codes_hbm.shape[2]
    layers = base_ref.shape[0]
    per_layer = codes_hbm.shape[0] // layers
    loads = [pltpu.make_async_copy(part, held.at[behind(me, o)], sems.at[p]) for p, (part, o) in enumerate(zip(parts, OFFSETS))]
    for load in loads:
        load.start()
    zero_code[...] = jnp.zeros_like(zero_code)
    zero_scale[...] = jnp.zeros_like(zero_scale)

    def clear(slot):
        return (
            pltpu.make_async_copy(zero_code, codes_hbm.at[slot], zero_sem.at[0]),
            pltpu.make_async_copy(zero_scale, scale_hbm.at[slot], zero_sem.at[1]),
        )

    def each_empty(act):
        def layer_step(layer, carry):
            for k in range(per_layer):

                @pl.when(k >= used_ref[layer])
                def _(k=k):
                    for copy in clear(per_layer * layer + k):
                        act(copy)

            return carry

        lax.fori_loop(0, layers, layer_step, 0)

    each_empty(lambda copy: copy.start())
    for load in loads:
        load.wait()

    def compute(j, code, scale):
        join_slot(held, j, FIRST, j, code, scale, width)

    write_slots(base_ref, used_ref, codes_hbm, scale_hbm, code_ref, scale_ref, code_sem, scale_sem, 0, FIRST, compute)
    each_empty(lambda copy: copy.wait())


def join_last_kernel(me_ref, base_ref, used_ref, *refs):
    peers = len(OFFSETS)
    parts, third_hbm, (codes_hbm, scale_hbm) = refs[:peers], refs[peers], refs[peers + 3 : peers + 5]
    held, code_ref, scale_ref, sems, code_sem, scale_sem = refs[peers + 5 :]
    me, width = me_ref[0], codes_hbm.shape[2]
    layers = base_ref.shape[0]
    loads = [
        pltpu.make_async_copy(part, held.at[0, behind(me, o)], sems.at[p]) for p, (part, o) in enumerate(zip(parts, OFFSETS))
    ]
    for load in loads:
        load.start()
    total = base_ref[layers - 1] + used_ref[layers - 1]

    @pl.when(total > FIRST + EACH)
    def _():
        load = pltpu.make_async_copy(third_hbm, held.at[1], sems.at[peers])
        load.start()
        load.wait()

    for load in loads:
        load.wait()

    def compute(j, code, scale):
        n = j - FIRST
        join_slot(held.at[n >> 3], n & (EACH - 1), EACH, j & 31, code, scale, width)

    write_slots(
        base_ref, used_ref, codes_hbm, scale_hbm, code_ref, scale_ref, code_sem, scale_sem, FIRST, FIRST + 2 * EACH, compute
    )


def in_vmem():
    return pl.BlockSpec(memory_space=pltpu.VMEM)


def in_hbm():
    return pl.BlockSpec(memory_space=pltpu.HBM)


def anywhere():
    return pl.BlockSpec(memory_space=pl.ANY)


def hbm(value):
    return pltpu.with_memory_space_constraint(value, pltpu.HBM)


def in_smem():
    return pl.BlockSpec(memory_space=pltpu.SMEM)


def sent_to(value, offset):
    count = SIDES[0] * SIDES[1] * SIDES[2]
    return lax.ppermute(value, SERVE, [(i, ahead(i, offset)) for i in range(count)])


def shards(train_weights, row_offset, block_group):
    train_n = lax.axis_size("train")
    serve_n = lax.axis_size(SERVE)
    train_idx = lax.axis_index("train")
    serve_idx = lax.axis_index(SERVE).astype(jnp.int32)
    layers, buffer_len, columns = train_weights.shape
    rows_dev = buffer_len - 2 * SHIFT
    blocks_dev = block_group.shape[1]
    per_layer = (blocks_dev + serve_n - 1) // serve_n + 1
    slots = layers * per_layer
    width = columns * serve_n
    groups = block_group[:, :, 0]
    me = serve_idx.reshape(1)
    by_column = hbm(jnp.transpose(train_weights, (2, 0, 1)))

    tile = (columns, layers, LANES)
    edge = jax.ShapeDtypeStruct((layers + 1, SHIFT, LANES), BF16)
    head, tail = pl.pallas_call(
        edges_kernel,
        grid=(1,),
        in_specs=[
            in_smem(),
            pl.BlockSpec(tile, lambda i: (0, 0, 0)),
            pl.BlockSpec(tile, lambda i: (0, 0, (buffer_len - 2 * SHIFT) // LANES)),
        ],
        out_specs=[in_vmem(), in_vmem()],
        out_shape=[edge, edge],
        scratch_shapes=[pltpu.VMEM((layers, LANES, LANES), BF16)],
        compiler_params=pltpu.CompilerParams(vmem_limit_bytes=8 * MIB),
        cost_estimate=pl.CostEstimate(flops=10**8, bytes_accessed=10**6, transcendentals=0),
        name="edges",
    )(me, by_column, by_column)
    left = lax.ppermute(tail, "train", [(i, i + 1) for i in range(train_n - 1)])
    right = lax.ppermute(head, "train", [(i + 1, i) for i in range(train_n - 1)])

    steps = LANES // PACK
    planes, rest, table, count = pl.pallas_call(
        functools.partial(planes_kernel, slots),
        in_specs=[in_smem(), in_smem(), in_hbm()],
        out_specs=[in_vmem(), in_vmem(), in_smem(), in_smem()],
        out_shape=[
            jax.ShapeDtypeStruct((layers, LANES, buffer_len), BF16),
            jax.ShapeDtypeStruct((buffer_len, LANES), F32),
            jax.ShapeDtypeStruct((serve_n * slots,), jnp.int32),
            jax.ShapeDtypeStruct((serve_n,), jnp.int32),
        ],
        scratch_shapes=[
            pltpu.VMEM((columns + PACK - 4, layers, buffer_len), BF16),
            pltpu.SemaphoreType.DMA((steps + 2,)),
        ],
        compiler_params=pltpu.CompilerParams(vmem_limit_bytes=16 * MIB),
        cost_estimate=pl.CostEstimate(flops=3 * 10**9, bytes_accessed=9 * 10**6, transcendentals=0),
        name="planes",
    )(me, groups, by_column)

    entries = jnp.arange(train_n + 1, dtype=jnp.int32)
    first_row = jnp.sum(jnp.where(entries[None, :] == train_idx, row_offset, 0), axis=1) - train_idx * rows_dev
    next_row = jnp.sum(jnp.where(entries[None, :] == train_idx + 1, row_offset, 0), axis=1) - train_idx * rows_dev
    peers = len(OFFSETS)
    first_set = jax.ShapeDtypeStruct((FIRST + 1, BLOCK, LANES), BF16)
    second_set = jax.ShapeDtypeStruct((EACH + 1, BLOCK, LANES), BF16)
    third_set = jax.ShapeDtypeStruct((serve_n, EACH + 1, BLOCK, LANES), BF16)
    packed = pl.pallas_call(
        functools.partial(pack_kernel, slots),
        in_specs=[in_smem()] * 5 + [in_vmem()] * 4,
        out_specs=[in_vmem()] * (2 * peers + 1),
        out_shape=[first_set] * peers + [second_set] * peers + [third_set],
        scratch_shapes=[pltpu.VMEM((layers, buffer_len, LANES), BF16), pltpu.VMEM((buffer_len, LANES), F32)],
        compiler_params=pltpu.CompilerParams(vmem_limit_bytes=24 * MIB),
        cost_estimate=pl.CostEstimate(flops=10**9, bytes_accessed=10**7, transcendentals=0),
        name="pack",
    )(me, first_row, next_row, table, count, planes, rest, left, right)

    got_first = [sent_to(v, o) for v, o in zip(packed[: peers - 1], OFFSETS)] + [packed[peers - 1]]
    got_second = [sent_to(v, o) for v, o in zip(packed[peers : 2 * peers - 1], OFFSETS)] + [packed[2 * peers - 1]]
    got_third = lax.cond(
        jnp.max(count) > FIRST + EACH,
        lambda v: lax.all_to_all(v, SERVE, split_axis=0, concat_axis=0, tiled=True),
        lambda v: v,
        packed[2 * peers],
    )

    used = jnp.sum((groups == serve_idx).astype(jnp.int32), axis=1)
    order = jnp.arange(layers, dtype=jnp.int32)
    base = jnp.sum(jnp.where(order[None, :] < order[:, None], used[None, :], 0), axis=1)
    ring = 4
    results = [pltpu.HBM((slots, BLOCK, width), BF16), pltpu.HBM((slots, 1, width), F32)]
    buffers = [pltpu.VMEM((ring, BLOCK, width), BF16), pltpu.VMEM((ring, 1, width), F32)]
    codes, scales = pl.pallas_call(
        join_first_kernel,
        in_specs=[in_smem()] * 3 + [anywhere()] * peers,
        out_specs=[in_hbm(), in_hbm()],
        out_shape=results,
        scratch_shapes=[
            pltpu.VMEM((serve_n, FIRST + 1, BLOCK, LANES), BF16),
            *buffers,
            pltpu.VMEM((BLOCK, width), BF16),
            pltpu.VMEM((1, width), F32),
            pltpu.SemaphoreType.DMA((peers,)),
            pltpu.SemaphoreType.DMA((ring,)),
            pltpu.SemaphoreType.DMA((ring,)),
            pltpu.SemaphoreType.DMA((2,)),
        ],
        compiler_params=pltpu.CompilerParams(vmem_limit_bytes=16 * MIB),
        cost_estimate=pl.CostEstimate(flops=4 * 10**9, bytes_accessed=10**7, transcendentals=0),
        name="join_first",
    )(me, base, used, *got_first)
    codes, scales = pl.pallas_call(
        join_last_kernel,
        in_specs=[in_smem()] * 3 + [anywhere()] * (peers + 1) + [in_hbm()] * 2,
        out_specs=[in_hbm(), in_hbm()],
        out_shape=results,
        input_output_aliases={peers + 4: 0, peers + 5: 1},
        scratch_shapes=[
            pltpu.VMEM((2, serve_n, EACH + 1, BLOCK, LANES), BF16),
            *buffers,
            pltpu.SemaphoreType.DMA((peers + 1,)),
            pltpu.SemaphoreType.DMA((ring,)),
            pltpu.SemaphoreType.DMA((ring,)),
        ],
        compiler_params=pltpu.CompilerParams(vmem_limit_bytes=16 * MIB),
        cost_estimate=pl.CostEstimate(flops=10**9, bytes_accessed=10**7, transcendentals=0),
        name="join_last",
    )(me, base, used, *got_second, got_third, codes, scales)
    return (
        codes.reshape(layers, 1, 1, per_layer, BLOCK, width),
        scales.reshape(layers, 1, 1, per_layer, width),
    )


def solution(mesh):
    finer = Mesh(mesh.devices.reshape(mesh.shape["train"], *SIDES), ("train", *SERVE))
    return jax.shard_map(
        shards,
        mesh=finer,
        in_specs=(P(None, "train", SERVE), P(), P(None, "train", None)),
        out_specs=(P(None, SERVE, "train", None, None, None), P(None, SERVE, "train", None, None)),
        check_vma=False,
    )
```

```python
import functools

import jax
import jax.numpy as jnp
from jax import lax
from jax.experimental import pallas as pl
from jax.experimental.pallas import tpu as pltpu
from jax.sharding import Mesh
from jax.sharding import PartitionSpec as P


BLOCK = 32
SHIFT = 32
LANES = 128
PACK = 16
SERVE = ("x", "y", "core")
SIDES = (2, 4, 2)
OFFSETS = [(dx, dy, dc) for dx, dy in ((1, 2), (1, 1), (1, 3), (0, 2), (1, 0), (0, 1), (0, 3), (0, 0)) for dc in (1, 0)]
FIRST = 32
EACH = 8
NT = (((1,), (1,)), ((), ()))
F32 = jnp.float32
BF16 = jnp.bfloat16
MIB = 1024 * 1024


def iota(shape, dim):
    return lax.broadcasted_iota(jnp.int32, shape, dim)


def identity(n):
    return (iota((n, n), 0) == iota((n, n), 1)).astype(BF16)


def layer_major():
    out, src = iota((PACK * PACK, PACK * PACK), 0), iota((PACK * PACK, PACK * PACK), 1)
    return ((out // PACK == src % PACK) & (out % PACK == src // PACK)).astype(BF16)


def rest_major():
    out, src = iota((LANES, 4 * PACK), 0), iota((LANES, 4 * PACK), 1)
    return ((out // 4 == src % PACK) & (out % 4 == src // PACK)).astype(BF16)


def dot(a, b):
    return jnp.dot(a, b, preferred_element_type=F32)


def turn(eye, value):
    return lax.dot_general(eye, value, NT, preferred_element_type=F32)


def ahead(me, offset):
    dx, dy, dc = offset
    return (me ^ (8 * dx + dc)) & 9 | ((me >> 1) + dy & 3) << 1


def behind(me, offset):
    dx, dy, dc = offset
    return ahead(me, (dx, -dy & 3, dc))


def edges_kernel(me_ref, first_ref, last_ref, head_ref, tail_ref, planes):
    rows = 2 * SHIFT
    lane = iota((1, 1, LANES), 2)
    perm = layer_major()
    eye = (iota((rows, LANES), 0) == iota((rows, LANES), 1)).astype(BF16)
    zero = jnp.zeros((), BF16)

    def columns(start, count):
        first, last = first_ref[pl.ds(start, count)], last_ref[pl.ds(start, count)]
        return jnp.where(lane < SHIFT, first, jnp.where(lane < rows, last, zero)).reshape(count * PACK, LANES)

    for i in range(LANES // PACK):
        x = columns(PACK * i, PACK)
        planes[:, PACK * i : PACK * (i + 1), :] = dot(perm, x).astype(BF16).reshape(PACK, PACK, LANES)
    shift = 4 * me_ref[0]
    for layer in range(PACK):
        turned = pltpu.roll(turn(eye, planes[layer]), shift, 1).astype(BF16)
        head_ref[layer], tail_ref[layer] = turned[:SHIFT], turned[SHIFT:]
    turned = turn(eye, dot(rest_major(), columns(LANES, 4)).astype(BF16)).astype(BF16)
    head_ref[PACK], tail_ref[PACK] = turned[:SHIFT], turned[SHIFT:]


def planes_kernel(slots, me_ref, group_ref, x_hbm, planes_ref, rest_ref, table_ref, count_ref, x_ref, sems):
    length = x_ref.shape[2]
    steps = LANES // PACK
    spare = PACK - 4
    parts = [(LANES - spare, spare, 0)] + [(PACK * i, PACK, spare + PACK * i) for i in range(steps)]
    parts.append((LANES, 4, spare + LANES))
    copies = [
        pltpu.make_async_copy(x_hbm.at[pl.ds(src, n)], x_ref.at[pl.ds(dst, n)], sems.at[i])
        for i, (src, n, dst) in enumerate(parts)
    ]
    for copy in copies:
        copy.start()
    layers, blocks = group_ref.shape
    for g in range(count_ref.shape[0]):
        count_ref[g] = 0
    perm = layer_major()
    turns, part = me_ref[0] >> 2, 4 * (me_ref[0] & 3)
    copies[0].wait()
    for i in range(steps):
        copies[i + 1].wait()
        x = x_ref[pl.ds(spare + PACK * i - part, PACK)].reshape(PACK * PACK, length)
        at = pl.multiple_of(PACK * ((i + turns) & (steps - 1)), PACK)
        planes_ref[:, pl.ds(at, PACK), :] = dot(perm, x).astype(BF16).reshape(PACK, PACK, length)
        for layer in range(layers * i // steps, layers * (i + 1) // steps):
            for b in range(blocks):
                group = group_ref[layer, b]
                j = count_ref[group]
                count_ref[group] = j + 1
                table_ref[group * slots + j] = (layer << 10) + SHIFT + BLOCK * b
    copies[steps + 1].wait()
    rest = dot(rest_major(), x_ref[pl.ds(spare + LANES, 4)].reshape(4 * PACK, length)).astype(BF16)
    for start in range(0, length, 256):
        size = min(256, length - start)
        rest_ref[start : start + size, :] = turn(identity(size), rest[:, start : start + size])


def pack_kernel(
    slots, me_ref, first_ref, next_ref, table_ref, count_ref, planes_ref, rest_ref, left_ref, right_ref, *refs
):
    peers = len(OFFSETS)
    sets, third_ref, (rows_ref, extra_ref) = (refs[:peers], refs[peers : 2 * peers]), refs[2 * peers], refs[2 * peers + 1 :]
    layers, _, length = planes_ref.shape
    row = iota((BLOCK, LANES), 0)
    lane_group = iota((BLOCK, LANES), 1) >> 2
    me = me_ref[0]
    last = length - 2 * SHIFT

    def pair_step(layer, carry):
        rows_ref[layer] = jnp.transpose(planes_ref[layer])
        return carry

    lax.fori_loop(0, layers, pair_step, 0)

    def edge_step(layer, carry):
        first, after = carry
        start, end = first_ref[layer], next_ref[layer] - (last - SHIFT)
        rows_ref[layer, SHIFT : 2 * SHIFT] = jnp.where(row < start, left_ref[layer], rows_ref[layer, SHIFT : 2 * SHIFT])
        rows_ref[layer, last : last + SHIFT] = jnp.where(row >= end, right_ref[layer], rows_ref[layer, last : last + SHIFT])
        return jnp.where(lane_group == layer, start, first), jnp.where(lane_group == layer, end, after)

    nothing = jnp.zeros((BLOCK, LANES), jnp.int32)
    first, after = lax.fori_loop(0, layers, edge_step, (nothing, nothing), unroll=4)
    extra_ref[...] = rest_ref[...]
    extra_ref[SHIFT : 2 * SHIFT] = jnp.where(row < first, left_ref[layers].astype(F32), rest_ref[SHIFT : 2 * SHIFT])
    extra_ref[last : last + SHIFT] = jnp.where(row >= after, right_ref[layers].astype(F32), rest_ref[last : last + SHIFT])

    def fill(ref, group, start, size):
        used = count_ref[group]
        rest = jnp.zeros((BLOCK, LANES), F32)
        for n in range(size):
            j = start + n
            entry = jnp.where(j < used, table_ref[group * slots + j], SHIFT)
            layer, at = entry >> 10, pl.multiple_of(entry & 1023, BLOCK)
            ref[n] = rows_ref[layer, pl.ds(at, BLOCK), :]
            place = j + me & 31
            moved = pltpu.roll(extra_ref[pl.ds(at, BLOCK), :], 4 * (place - layer) & (LANES - 1), 1)
            rest = jnp.where(lane_group == place, moved, rest)
        ref[size] = rest.astype(BF16)

    for p, offset in enumerate(OFFSETS):
        group = ahead(me, offset)
        fill(sets[0][p], group, 0, FIRST)
        fill(sets[1][p], group, FIRST, EACH)

        @pl.when(count_ref[group] > FIRST + EACH)
        def _(group=group):
            fill(third_ref.at[group], group, FIRST + EACH, EACH)


def join_slot(held, n, tile, jj, code_ref, scale_ref, width):
    peers = held.shape[0]
    lane = iota((BLOCK, LANES), 1)
    source = (lane >> 2) - jj & 31
    rest = jnp.zeros((BLOCK, LANES), F32)
    for s in range(peers):
        rest = jnp.where(source == s, held[s, tile].astype(F32), rest)
    rest = pltpu.roll(rest, -4 * jj & (LANES - 1), 1)
    before = None
    for t in range(peers + 1):
        x = rest
        if before is not None:
            x = jnp.where(lane < 4 * t - 4, before, x)
        if t < peers:
            own = held[t, n].astype(F32)
            x = own if t == 0 else jnp.where(lane >= 4 * t, own, x)
            before = own
        size = min(LANES, width - LANES * t)
        top = jnp.maximum(jnp.max(jnp.abs(x), axis=0, keepdims=True), 0.25)
        scale_ref[:, LANES * t : LANES * t + size] = top[:, :size]
        code_ref[:, LANES * t : LANES * t + size] = (x * (1.0 / top)).astype(BF16)[:, :size]


def write_slots(base_ref, used_ref, codes_hbm, scale_hbm, code_ref, scale_ref, code_sem, scale_sem, low, high, compute):
    layers = base_ref.shape[0]
    per_layer = codes_hbm.shape[0] // layers
    ring = code_ref.shape[0]

    def stores(i, slot):
        return (
            pltpu.make_async_copy(code_ref.at[i], codes_hbm.at[slot], code_sem.at[i]),
            pltpu.make_async_copy(scale_ref.at[i], scale_hbm.at[slot], scale_sem.at[i]),
        )

    def layer_step(layer, done):
        for k in range(per_layer):
            j = base_ref[layer] + k
            mine = (k < used_ref[layer]) & (j >= low) & (j < high)
            i = done & (ring - 1)

            @pl.when(mine)
            def _(j=j, i=i, done=done, k=k):
                @pl.when(done >= ring)
                def _():
                    for store in stores(i, 0):
                        store.wait()

                compute(j, code_ref.at[i], scale_ref.at[i])
                for store in stores(i, per_layer * layer + k):
                    store.start()

            done = done + mine.astype(jnp.int32)
        return done

    done = lax.fori_loop(0, layers, layer_step, jnp.int32(0))
    for i in range(ring):

        @pl.when(done > i)
        def _(i=i):
            for store in stores(i, 0):
                store.wait()


def join_first_kernel(me_ref, base_ref, used_ref, *refs):
    peers = len(OFFSETS)
    parts, (codes_hbm, scale_hbm) = refs[:peers], refs[peers : peers + 2]
    held, code_ref, scale_ref, zero_code, zero_scale, sems, code_sem, scale_sem, zero_sem = refs[peers + 2 :]
    me, width = me_ref[0], codes_hbm.shape[2]
    layers = base_ref.shape[0]
    per_layer = codes_hbm.shape[0] // layers
    loads = [pltpu.make_async_copy(part, held.at[behind(me, o)], sems.at[p]) for p, (part, o) in enumerate(zip(parts, OFFSETS))]
    for load in loads:
        load.start()
    zero_code[...] = jnp.zeros_like(zero_code)
    zero_scale[...] = jnp.zeros_like(zero_scale)

    def clear(slot):
        return (
            pltpu.make_async_copy(zero_code, codes_hbm.at[slot], zero_sem.at[0]),
            pltpu.make_async_copy(zero_scale, scale_hbm.at[slot], zero_sem.at[1]),
        )

    def each_empty(act):
        def layer_step(layer, carry):
            for k in range(per_layer):

                @pl.when(k >= used_ref[layer])
                def _(k=k):
                    for copy in clear(per_layer * layer + k):
                        act(copy)

            return carry

        lax.fori_loop(0, layers, layer_step, 0)

    each_empty(lambda copy: copy.start())
    for load in loads:
        load.wait()

    def compute(j, code, scale):
        join_slot(held, j, FIRST, j, code, scale, width)

    write_slots(base_ref, used_ref, codes_hbm, scale_hbm, code_ref, scale_ref, code_sem, scale_sem, 0, FIRST, compute)
    each_empty(lambda copy: copy.wait())


def join_last_kernel(me_ref, base_ref, used_ref, *refs):
    peers = len(OFFSETS)
    parts, third_hbm, (codes_hbm, scale_hbm) = refs[:peers], refs[peers], refs[peers + 3 : peers + 5]
    held, code_ref, scale_ref, sems, code_sem, scale_sem = refs[peers + 5 :]
    me, width = me_ref[0], codes_hbm.shape[2]
    layers = base_ref.shape[0]
    loads = [
        pltpu.make_async_copy(part, held.at[0, behind(me, o)], sems.at[p]) for p, (part, o) in enumerate(zip(parts, OFFSETS))
    ]
    for load in loads:
        load.start()
    total = base_ref[layers - 1] + used_ref[layers - 1]

    @pl.when(total > FIRST + EACH)
    def _():
        load = pltpu.make_async_copy(third_hbm, held.at[1], sems.at[peers])
        load.start()
        load.wait()

    for load in loads:
        load.wait()

    def compute(j, code, scale):
        n = j - FIRST
        join_slot(held.at[n >> 3], n & (EACH - 1), EACH, j & 31, code, scale, width)

    write_slots(
        base_ref, used_ref, codes_hbm, scale_hbm, code_ref, scale_ref, code_sem, scale_sem, FIRST, FIRST + 2 * EACH, compute
    )


def in_vmem():
    return pl.BlockSpec(memory_space=pltpu.VMEM)


def in_hbm():
    return pl.BlockSpec(memory_space=pltpu.HBM)


def anywhere():
    return pl.BlockSpec(memory_space=pl.ANY)


def hbm(value):
    return pltpu.with_memory_space_constraint(value, pltpu.HBM)


def in_smem():
    return pl.BlockSpec(memory_space=pltpu.SMEM)


def sent_to(value, offset):
    count = SIDES[0] * SIDES[1] * SIDES[2]
    return lax.ppermute(value, SERVE, [(i, ahead(i, offset)) for i in range(count)])


def shards(train_weights, row_offset, block_group):
    train_n = lax.axis_size("train")
    serve_n = lax.axis_size(SERVE)
    train_idx = lax.axis_index("train")
    serve_idx = lax.axis_index(SERVE).astype(jnp.int32)
    layers, buffer_len, columns = train_weights.shape
    rows_dev = buffer_len - 2 * SHIFT
    blocks_dev = block_group.shape[1]
    per_layer = (blocks_dev + serve_n - 1) // serve_n + 1
    slots = layers * per_layer
    width = columns * serve_n
    groups = block_group[:, :, 0]
    me = serve_idx.reshape(1)
    by_column = hbm(jnp.transpose(train_weights, (2, 0, 1)))

    tile = (columns, layers, LANES)
    edge = jax.ShapeDtypeStruct((layers + 1, SHIFT, LANES), BF16)
    head, tail = pl.pallas_call(
        edges_kernel,
        grid=(1,),
        in_specs=[
            in_smem(),
            pl.BlockSpec(tile, lambda i: (0, 0, 0)),
            pl.BlockSpec(tile, lambda i: (0, 0, (buffer_len - 2 * SHIFT) // LANES)),
        ],
        out_specs=[in_vmem(), in_vmem()],
        out_shape=[edge, edge],
        scratch_shapes=[pltpu.VMEM((layers, LANES, LANES), BF16)],
        compiler_params=pltpu.CompilerParams(vmem_limit_bytes=8 * MIB),
        cost_estimate=pl.CostEstimate(flops=10**8, bytes_accessed=10**6, transcendentals=0),
        name="edges",
    )(me, by_column, by_column)
    left = lax.ppermute(tail, "train", [(i, i + 1) for i in range(train_n - 1)])
    right = lax.ppermute(head, "train", [(i + 1, i) for i in range(train_n - 1)])

    steps = LANES // PACK
    planes, rest, table, count = pl.pallas_call(
        functools.partial(planes_kernel, slots),
        in_specs=[in_smem(), in_smem(), in_hbm()],
        out_specs=[in_vmem(), in_vmem(), in_smem(), in_smem()],
        out_shape=[
            jax.ShapeDtypeStruct((layers, LANES, buffer_len), BF16),
            jax.ShapeDtypeStruct((buffer_len, LANES), F32),
            jax.ShapeDtypeStruct((serve_n * slots,), jnp.int32),
            jax.ShapeDtypeStruct((serve_n,), jnp.int32),
        ],
        scratch_shapes=[
            pltpu.VMEM((columns + PACK - 4, layers, buffer_len), BF16),
            pltpu.SemaphoreType.DMA((steps + 2,)),
        ],
        compiler_params=pltpu.CompilerParams(vmem_limit_bytes=16 * MIB),
        cost_estimate=pl.CostEstimate(flops=3 * 10**9, bytes_accessed=9 * 10**6, transcendentals=0),
        name="planes",
    )(me, groups, by_column)

    entries = jnp.arange(train_n + 1, dtype=jnp.int32)
    first_row = jnp.sum(jnp.where(entries[None, :] == train_idx, row_offset, 0), axis=1) - train_idx * rows_dev
    next_row = jnp.sum(jnp.where(entries[None, :] == train_idx + 1, row_offset, 0), axis=1) - train_idx * rows_dev
    peers = len(OFFSETS)
    first_set = jax.ShapeDtypeStruct((FIRST + 1, BLOCK, LANES), BF16)
    second_set = jax.ShapeDtypeStruct((EACH + 1, BLOCK, LANES), BF16)
    third_set = jax.ShapeDtypeStruct((serve_n, EACH + 1, BLOCK, LANES), BF16)
    packed = pl.pallas_call(
        functools.partial(pack_kernel, slots),
        in_specs=[in_smem()] * 5 + [in_vmem()] * 4,
        out_specs=[in_vmem()] * (2 * peers + 1),
        out_shape=[first_set] * peers + [second_set] * peers + [third_set],
        scratch_shapes=[pltpu.VMEM((layers, buffer_len, LANES), BF16), pltpu.VMEM((buffer_len, LANES), F32)],
        compiler_params=pltpu.CompilerParams(vmem_limit_bytes=24 * MIB),
        cost_estimate=pl.CostEstimate(flops=10**9, bytes_accessed=10**7, transcendentals=0),
        name="pack",
    )(me, first_row, next_row, table, count, planes, rest, left, right)

    got_first = [sent_to(v, o) for v, o in zip(packed[: peers - 1], OFFSETS)] + [packed[peers - 1]]
    got_second = [sent_to(v, o) for v, o in zip(packed[peers : 2 * peers - 1], OFFSETS)] + [packed[2 * peers - 1]]
    got_third = lax.cond(
        jnp.max(count) > FIRST + EACH,
        lambda v: lax.all_to_all(v, SERVE, split_axis=0, concat_axis=0, tiled=True),
        lambda v: v,
        packed[2 * peers],
    )

    used = jnp.sum((groups == serve_idx).astype(jnp.int32), axis=1)
    order = jnp.arange(layers, dtype=jnp.int32)
    base = jnp.sum(jnp.where(order[None, :] < order[:, None], used[None, :], 0), axis=1)
    ring = 4
    results = [pltpu.HBM((slots, BLOCK, width), BF16), pltpu.HBM((slots, 1, width), F32)]
    buffers = [pltpu.VMEM((ring, BLOCK, width), BF16), pltpu.VMEM((ring, 1, width), F32)]
    codes, scales = pl.pallas_call(
        join_first_kernel,
        in_specs=[in_smem()] * 3 + [anywhere()] * peers,
        out_specs=[in_hbm(), in_hbm()],
        out_shape=results,
        scratch_shapes=[
            pltpu.VMEM((serve_n, FIRST + 1, BLOCK, LANES), BF16),
            *buffers,
            pltpu.VMEM((BLOCK, width), BF16),
            pltpu.VMEM((1, width), F32),
            pltpu.SemaphoreType.DMA((peers,)),
            pltpu.SemaphoreType.DMA((ring,)),
            pltpu.SemaphoreType.DMA((ring,)),
            pltpu.SemaphoreType.DMA((2,)),
        ],
        compiler_params=pltpu.CompilerParams(vmem_limit_bytes=16 * MIB),
        cost_estimate=pl.CostEstimate(flops=4 * 10**9, bytes_accessed=10**7, transcendentals=0),
        name="join_first",
    )(me, base, used, *got_first)
    codes, scales = pl.pallas_call(
        join_last_kernel,
        in_specs=[in_smem()] * 3 + [anywhere()] * (peers + 1) + [in_hbm()] * 2,
        out_specs=[in_hbm(), in_hbm()],
        out_shape=results,
        input_output_aliases={peers + 4: 0, peers + 5: 1},
        scratch_shapes=[
            pltpu.VMEM((2, serve_n, EACH + 1, BLOCK, LANES), BF16),
            *buffers,
            pltpu.SemaphoreType.DMA((peers + 1,)),
            pltpu.SemaphoreType.DMA((ring,)),
            pltpu.SemaphoreType.DMA((ring,)),
        ],
        compiler_params=pltpu.CompilerParams(vmem_limit_bytes=16 * MIB),
        cost_estimate=pl.CostEstimate(flops=10**9, bytes_accessed=10**7, transcendentals=0),
        name="join_last",
    )(me, base, used, *got_second, got_third, codes, scales)
    return (
        codes.reshape(layers, 1, 1, per_layer, BLOCK, width),
        scales.reshape(layers, 1, 1, per_layer, width),
    )


def solution(mesh):
    finer = Mesh(mesh.devices.reshape(mesh.shape["train"], *SIDES), ("train", *SERVE))
    return jax.shard_map(
        shards,
        mesh=finer,
        in_specs=(P(None, "train", SERVE), P(), P(None, "train", None)),
        out_specs=(P(None, SERVE, "train", None, None, None), P(None, SERVE, "train", None, None)),
        check_vma=False,
    )
```

```python
import jax
import jax.numpy as jnp
from jax import lax
from jax.experimental import pallas as pl
from jax.experimental.pallas import tpu as pltpu
from jax.sharding import Mesh
from jax.sharding import PartitionSpec as P


BLOCK = 32
SHIFT = 32
LANES = 128
PACK = 16
SERVE = ("x", "y", "core")
SIDES = (2, 4, 2)
OFFSETS = [
    (dx, dy, dc)
    for dx, dy in ((1, 2), (0, 1), (1, 1), (0, 3), (0, 2), (1, 3), (1, 0), (0, 0))
    for dc in (1, 0)
]
LATER = sorted(range(len(OFFSETS)), key=lambda p: (-OFFSETS[p][0], p))
FIRST, SECOND, THIRD = 28, 12, 20
ENTRIES = 64
NT = (((1,), (1,)), ((), ()))
F32 = jnp.float32
BF16 = jnp.bfloat16
MIB = 1024 * 1024


def iota(shape, dim):
    return lax.broadcasted_iota(jnp.int32, shape, dim)


def identity(n):
    return (iota((n, n), 0) == iota((n, n), 1)).astype(BF16)


def layer_major():
    out, src = iota((PACK * PACK, PACK * PACK), 0), iota((PACK * PACK, PACK * PACK), 1)
    return ((out // PACK == src % PACK) & (out % PACK == src // PACK)).astype(BF16)


def rest_major():
    out, src = iota((LANES, 4 * PACK), 0), iota((LANES, 4 * PACK), 1)
    return ((out // 4 == src % PACK) & (out % 4 == src // PACK)).astype(BF16)


def dot(a, b):
    return jnp.dot(a, b, preferred_element_type=F32)


def turn(eye, value):
    return lax.dot_general(eye, value, NT, preferred_element_type=F32)


def ahead(me, offset):
    dx, dy, dc = offset
    return (me ^ (8 * dx + dc)) & 9 | ((me >> 1) + dy & 3) << 1


def behind(me, offset):
    dx, dy, dc = offset
    return ahead(me, (dx, -dy & 3, dc))


def fill(refs, me, group, start, size, end, block, ref):
    table_ref, extra_ref = refs
    lane_group = iota((BLOCK, LANES), 1) >> 2
    rest = jnp.zeros((BLOCK, LANES), F32)
    for n in range(size):
        j = start + n
        entry = jnp.where(j < end, table_ref[group * ENTRIES + j], SHIFT)
        layer, at = entry >> 10, pl.multiple_of(entry & 1023, BLOCK)
        ref[n] = block(layer, at)
        place = j + me & 31
        moved = pltpu.roll(extra_ref[pl.ds(at, BLOCK), :], 4 * (place - layer) & (LANES - 1), 1)
        rest = jnp.where(lane_group == place, moved, rest)
    ref[size] = rest.astype(BF16)


def turn_kernel(me_ref, group_ref, x_hbm, *refs):
    peers = len(OFFSETS)
    first_set, (rows_hbm, extra_ref, head_ref, tail_ref, table_ref, inner_ref, end_ref) = refs[:peers], refs[peers : peers + 7]
    x_ref, planes, rows_ref, sems, out_sem = refs[peers + 7 :]
    length = x_ref.shape[2]
    steps = LANES // PACK
    spare = PACK - 4
    parts = [(LANES - spare, spare, 0)] + [(PACK * i, PACK, spare + PACK * i) for i in range(steps)]
    parts.append((LANES, 4, spare + LANES))
    copies = [
        pltpu.make_async_copy(x_hbm.at[pl.ds(src, n)], x_ref.at[pl.ds(dst, n)], sems.at[i])
        for i, (src, n, dst) in enumerate(parts)
    ]
    for copy in copies:
        copy.start()
    layers, blocks = group_ref.shape
    groups = inner_ref.shape[0]

    def enter(count_ref, layer, b):
        group = group_ref[layer, b]
        j = count_ref[group]
        count_ref[group] = j + 1
        table_ref[group * ENTRIES + j] = (layer << 10) + SHIFT + BLOCK * b

    for g in range(groups):
        inner_ref[g] = 0
    perm = layer_major()
    me = me_ref[0]
    turns, part = me >> 2, 4 * (me & 3)
    copies[0].wait()
    for i in range(steps):
        copies[i + 1].wait()
        x = x_ref[pl.ds(spare + PACK * i - part, PACK)].reshape(PACK * PACK, length)
        at = pl.multiple_of(PACK * ((i + turns) & (steps - 1)), PACK)
        planes[:, pl.ds(at, PACK), :] = dot(perm, x).astype(BF16).reshape(PACK, PACK, length)
        for layer in range(layers * i // steps, layers * (i + 1) // steps):
            for b in range(1, blocks - 1):
                enter(inner_ref, layer, b)
    copies[steps + 1].wait()
    rest = dot(rest_major(), x_ref[pl.ds(spare + LANES, 4)].reshape(4 * PACK, length)).astype(BF16)
    for start in range(0, length, 256):
        size = min(256, length - start)
        extra_ref[start : start + size, :] = turn(identity(size), rest[:, start : start + size])
    for g in range(groups):
        end_ref[g] = jnp.maximum(inner_ref[g], FIRST)
    for layer in range(layers):
        for b in (0, blocks - 1):
            enter(end_ref, layer, b)

    def layer_step(layer, carry):
        turned = jnp.transpose(planes[layer])
        rows_ref[layer] = turned
        head_ref[layer] = turned[:SHIFT]
        tail_ref[layer] = turned[length - SHIFT :]
        pltpu.make_async_copy(rows_ref.at[layer], rows_hbm.at[layer], out_sem).start()
        return carry

    lax.fori_loop(0, layers, layer_step, 0)
    head_ref[layers] = extra_ref[:SHIFT].astype(BF16)
    tail_ref[layers] = extra_ref[length - SHIFT :].astype(BF16)
    for p, offset in enumerate(OFFSETS):
        group = ahead(me, offset)
        fill(
            (table_ref, extra_ref), me, group, 0, FIRST, inner_ref[group],
            lambda layer, at: rows_ref[layer, pl.ds(at, BLOCK), :], first_set[p],
        )
    pltpu.make_async_copy(rows_ref, rows_hbm, out_sem).wait()


def rest_kernel(me_ref, shard_ref, offset_ref, table_ref, end_ref, rows_hbm, rest_ref, left_ref, right_ref, *refs):
    peers = len(OFFSETS)
    second_set, third_ref, (rows_ref, edge_ref, extra_ref, sem) = refs[:peers], refs[peers], refs[peers + 1 :]
    load = pltpu.make_async_copy(rows_hbm, rows_ref, sem)
    load.start()
    load.wait()
    layers, length = rows_ref.shape[:2]
    row = iota((BLOCK, LANES), 0)
    lane_group = iota((BLOCK, LANES), 1) >> 2
    me, shard = me_ref[0], shard_ref[0]
    last = length - 2 * SHIFT
    before = shard * (length - 2 * SHIFT)

    def edge_step(layer, carry):
        first, after = carry
        start = offset_ref[layer, shard] - before
        end = offset_ref[layer, shard + 1] - before - (last - SHIFT)
        edge_ref[layer, :SHIFT] = jnp.where(row < start, left_ref[layer], rows_ref[layer, SHIFT : 2 * SHIFT])
        edge_ref[layer, SHIFT:] = jnp.where(row >= end, right_ref[layer], rows_ref[layer, last : last + SHIFT])
        return jnp.where(lane_group == layer, start, first), jnp.where(lane_group == layer, end, after)

    nothing = jnp.zeros((BLOCK, LANES), jnp.int32)
    first, after = lax.fori_loop(0, layers, edge_step, (nothing, nothing), unroll=4)
    extra_ref[...] = rest_ref[...]
    extra_ref[SHIFT : 2 * SHIFT] = jnp.where(row < first, left_ref[layers].astype(F32), rest_ref[SHIFT : 2 * SHIFT])
    extra_ref[last : last + SHIFT] = jnp.where(row >= after, right_ref[layers].astype(F32), rest_ref[last : last + SHIFT])

    def block(layer, at):
        low, high = at == SHIFT, at == last
        edge = edge_ref[layer, pl.ds(pl.multiple_of(jnp.where(high, SHIFT, 0), BLOCK), BLOCK), :]
        return jnp.where(low | high, edge, rows_ref[layer, pl.ds(at, BLOCK), :])

    for p, offset in enumerate(OFFSETS):
        group = ahead(me, offset)
        fill((table_ref, extra_ref), me, group, FIRST, SECOND, end_ref[group], block, second_set[p])

    def third_step(group, carry):
        @pl.when(end_ref[group] > FIRST + SECOND)
        def _():
            fill((table_ref, extra_ref), me, group, FIRST + SECOND, THIRD, end_ref[group], block, third_ref.at[group])

        return carry

    lax.fori_loop(0, peers, third_step, 0)


def join_slot(held, n, tile, jj, code_ref, scale_ref, width):
    peers = held.shape[0]
    lane = iota((BLOCK, LANES), 1)
    source = (lane >> 2) - jj & 31
    rest = jnp.zeros((BLOCK, LANES), F32)
    for s in range(peers):
        rest = jnp.where(source == s, held[s, tile].astype(F32), rest)
    rest = pltpu.roll(rest, -4 * jj & (LANES - 1), 1)
    before = None
    for t in range(peers + 1):
        x = rest
        if before is not None:
            x = jnp.where(lane < 4 * t - 4, before, x)
        if t < peers:
            own = held[t, n].astype(F32)
            x = own if t == 0 else jnp.where(lane >= 4 * t, own, x)
            before = own
        size = min(LANES, width - LANES * t)
        top = jnp.maximum(jnp.max(jnp.abs(x), axis=0, keepdims=True), 0.25)
        scale_ref[:, LANES * t : LANES * t + size] = top[:, :size]
        code_ref[:, LANES * t : LANES * t + size] = (x * (1.0 / top)).astype(BF16)[:, :size]


def write_slots(slot_ref, used_ref, codes_hbm, scale_hbm, code_ref, scale_ref, code_sem, scale_sem, low, high, compute):
    layers = used_ref.shape[0]
    per_layer = codes_hbm.shape[0] // layers
    ring = code_ref.shape[0]

    def stores(i, slot):
        return (
            pltpu.make_async_copy(code_ref.at[i], codes_hbm.at[slot], code_sem.at[i]),
            pltpu.make_async_copy(scale_ref.at[i], scale_hbm.at[slot], scale_sem.at[i]),
        )

    def layer_step(layer, done):
        for k in range(per_layer):
            j = slot_ref[per_layer * layer + k]
            mine = (k < used_ref[layer]) & (j >= low) & (j < high)
            i = done & (ring - 1)

            @pl.when(mine)
            def _(j=j, i=i, done=done, k=k):
                @pl.when(done >= ring)
                def _():
                    for store in stores(i, 0):
                        store.wait()

                compute(j, code_ref.at[i], scale_ref.at[i])
                for store in stores(i, per_layer * layer + k):
                    store.start()

            done = done + mine.astype(jnp.int32)
        return done

    done = lax.fori_loop(0, layers, layer_step, jnp.int32(0))
    for i in range(ring):

        @pl.when(done > i)
        def _(i=i):
            for store in stores(i, 0):
                store.wait()


def join_first_kernel(me_ref, group_ref, inner_ref, *refs):
    peers = len(OFFSETS)
    parts, (codes_hbm, scale_hbm, slot_ref, used_ref) = refs[:peers], refs[peers : peers + 4]
    held, code_ref, scale_ref, zero_code, zero_scale, sems, code_sem, scale_sem, zero_sem = refs[peers + 4 :]
    me, width = me_ref[0], codes_hbm.shape[2]
    layers, blocks = group_ref.shape
    per_layer = codes_hbm.shape[0] // layers
    loads = [pltpu.make_async_copy(part, held.at[behind(me, o)], sems.at[p]) for p, (part, o) in enumerate(zip(parts, OFFSETS))]
    for load in loads:
        load.start()
    zero_code[...] = jnp.zeros_like(zero_code)
    zero_scale[...] = jnp.zeros_like(zero_scale)

    def find(layer, carry):
        inner, edge = carry
        k = jnp.int32(0)
        for b in range(blocks):
            mine = (group_ref[layer, b] == me).astype(jnp.int32)
            at_edge = b in (0, blocks - 1)
            slot_ref[jnp.where(mine == 1, per_layer * layer + k, per_layer * layers)] = edge if at_edge else inner
            k = k + mine
            inner, edge = (inner, edge + mine) if at_edge else (inner + mine, edge)
        used_ref[layer] = k
        return inner, edge

    lax.fori_loop(0, layers, find, (jnp.int32(0), jnp.maximum(inner_ref[me], FIRST)))

    def clear(slot):
        return (
            pltpu.make_async_copy(zero_code, codes_hbm.at[slot], zero_sem.at[0]),
            pltpu.make_async_copy(zero_scale, scale_hbm.at[slot], zero_sem.at[1]),
        )

    def each_empty(act):
        def layer_step(layer, carry):
            for k in range(per_layer):

                @pl.when(k >= used_ref[layer])
                def _(k=k):
                    for copy in clear(per_layer * layer + k):
                        act(copy)

            return carry

        lax.fori_loop(0, layers, layer_step, 0)

    each_empty(lambda copy: copy.start())
    for load in loads:
        load.wait()

    def compute(j, code, scale):
        join_slot(held, j, FIRST, j, code, scale, width)

    write_slots(slot_ref, used_ref, codes_hbm, scale_hbm, code_ref, scale_ref, code_sem, scale_sem, 0, FIRST, compute)
    each_empty(lambda copy: copy.wait())


def join_last_kernel(me_ref, slot_ref, used_ref, end_ref, *refs):
    peers = len(OFFSETS)
    parts, third_hbm, (codes_hbm, scale_hbm) = refs[:peers], refs[peers], refs[peers + 3 : peers + 5]
    held, code_ref, scale_ref, sems, code_sem, scale_sem = refs[peers + 5 :]
    me, width = me_ref[0], codes_hbm.shape[2]
    loads = [
        pltpu.make_async_copy(part, held.at[behind(me, o), pl.ds(0, SECOND + 1)], sems.at[p])
        for p, (part, o) in enumerate(zip(parts, OFFSETS))
    ]
    for load in loads:
        load.start()

    @pl.when(end_ref[me] > FIRST + SECOND)
    def _():
        load = pltpu.make_async_copy(third_hbm, held.at[:, pl.ds(SECOND + 1, THIRD + 1)], sems.at[peers])
        load.start()
        load.wait()

    for load in loads:
        load.wait()

    def compute(j, code, scale):
        late = (j >= FIRST + SECOND).astype(jnp.int32)
        join_slot(held, j - FIRST + late, SECOND + late * (THIRD + 1), j & 31, code, scale, width)

    write_slots(
        slot_ref, used_ref, codes_hbm, scale_hbm, code_ref, scale_ref, code_sem, scale_sem, FIRST, ENTRIES, compute
    )


def in_vmem():
    return pl.BlockSpec(memory_space=pltpu.VMEM)


def in_hbm():
    return pl.BlockSpec(memory_space=pltpu.HBM)


def anywhere():
    return pl.BlockSpec(memory_space=pl.ANY)


def hbm(value):
    return pltpu.with_memory_space_constraint(value, pltpu.HBM)


def in_smem():
    return pl.BlockSpec(memory_space=pltpu.SMEM)


def sent_to(value, offset):
    count = SIDES[0] * SIDES[1] * SIDES[2]
    return lax.ppermute(value, SERVE, [(i, ahead(i, offset)) for i in range(count)])


def shards(train_weights, row_offset, block_group):
    train_n = lax.axis_size("train")
    serve_n = lax.axis_size(SERVE)
    train_idx = lax.axis_index("train")
    serve_idx = lax.axis_index(SERVE).astype(jnp.int32)
    layers, buffer_len, columns = train_weights.shape
    blocks_dev = block_group.shape[1]
    per_layer = (blocks_dev + serve_n - 1) // serve_n + 1
    slots = layers * per_layer
    width = columns * serve_n
    groups = block_group[:, :, 0]
    me, shard = serve_idx.reshape(1), train_idx.astype(jnp.int32).reshape(1)
    by_column = hbm(jnp.transpose(train_weights, (2, 0, 1)))

    peers = len(OFFSETS)
    steps = LANES // PACK
    edge = jax.ShapeDtypeStruct((layers + 1, SHIFT, LANES), BF16)
    per_group = jax.ShapeDtypeStruct((serve_n,), jnp.int32)
    turned = pl.pallas_call(
        turn_kernel,
        in_specs=[in_smem(), in_smem(), in_hbm()],
        out_specs=[in_vmem()] * peers + [in_hbm()] + [in_vmem()] * 3 + [in_smem()] * 3,
        out_shape=[jax.ShapeDtypeStruct((FIRST + 1, BLOCK, LANES), BF16)] * peers
        + [
            pltpu.HBM((layers, buffer_len, LANES), BF16),
            jax.ShapeDtypeStruct((buffer_len, LANES), F32),
            edge,
            edge,
            jax.ShapeDtypeStruct((serve_n * ENTRIES,), jnp.int32),
            per_group,
            per_group,
        ],
        scratch_shapes=[
            pltpu.VMEM((columns + PACK - 4, layers, buffer_len), BF16),
            pltpu.VMEM((layers, LANES, buffer_len), BF16),
            pltpu.VMEM((layers, buffer_len, LANES), BF16),
            pltpu.SemaphoreType.DMA((steps + 2,)),
            pltpu.SemaphoreType.DMA,
        ],
        compiler_params=pltpu.CompilerParams(vmem_limit_bytes=24 * MIB),
        cost_estimate=pl.CostEstimate(flops=3 * 10**9, bytes_accessed=9 * 10**6, transcendentals=0),
        name="turn",
    )(me, groups, by_column)
    first_sent, (rows, rest, head, tail, table, inner, end) = turned[:peers], turned[peers:]
    left = lax.ppermute(tail, "train", [(i, i + 1) for i in range(train_n - 1)])
    right = lax.ppermute(head, "train", [(i + 1, i) for i in range(train_n - 1)])
    *second_sent, third_sent = pl.pallas_call(
        rest_kernel,
        in_specs=[in_smem()] * 5 + [in_hbm()] + [in_vmem()] * 3,
        out_specs=[in_vmem()] * (peers + 1),
        out_shape=[jax.ShapeDtypeStruct((SECOND + 1, BLOCK, LANES), BF16)] * peers
        + [jax.ShapeDtypeStruct((serve_n, THIRD + 1, BLOCK, LANES), BF16)],
        scratch_shapes=[
            pltpu.VMEM((layers, buffer_len, LANES), BF16),
            pltpu.VMEM((layers, 2 * SHIFT, LANES), BF16),
            pltpu.VMEM((buffer_len, LANES), F32),
            pltpu.SemaphoreType.DMA,
        ],
        compiler_params=pltpu.CompilerParams(vmem_limit_bytes=16 * MIB),
        cost_estimate=pl.CostEstimate(flops=10**9, bytes_accessed=10**7, transcendentals=0),
        name="rest",
    )(me, shard, row_offset, table, end, hbm(rows), rest, left, right)

    got_first = [sent_to(v, o) for v, o in zip(first_sent[:-1], OFFSETS)] + [first_sent[-1]]
    got_second = list(second_sent)
    for p in LATER:
        if p < peers - 1:
            got_second[p] = sent_to(second_sent[p], OFFSETS[p])
    got_third = lax.cond(
        jnp.max(end) > FIRST + SECOND,
        lambda v: lax.all_to_all(v, SERVE, split_axis=0, concat_axis=0, tiled=True),
        lambda v: v,
        third_sent,
    )
    ring = 4
    results = [pltpu.HBM((slots, BLOCK, width), BF16), pltpu.HBM((slots, 1, width), F32)]
    buffers = [pltpu.VMEM((ring, BLOCK, width), BF16), pltpu.VMEM((ring, 1, width), F32)]
    codes, scales, slot_of, used = pl.pallas_call(
        join_first_kernel,
        in_specs=[in_smem()] * 3 + [anywhere()] * peers,
        out_specs=[in_hbm(), in_hbm(), in_smem(), in_smem()],
        out_shape=results
        + [jax.ShapeDtypeStruct((slots + 1,), jnp.int32), jax.ShapeDtypeStruct((layers,), jnp.int32)],
        scratch_shapes=[
            pltpu.VMEM((serve_n, FIRST + 1, BLOCK, LANES), BF16),
            *buffers,
            pltpu.VMEM((BLOCK, width), BF16),
            pltpu.VMEM((1, width), F32),
            pltpu.SemaphoreType.DMA((peers,)),
            pltpu.SemaphoreType.DMA((ring,)),
            pltpu.SemaphoreType.DMA((ring,)),
            pltpu.SemaphoreType.DMA((2,)),
        ],
        compiler_params=pltpu.CompilerParams(vmem_limit_bytes=16 * MIB),
        cost_estimate=pl.CostEstimate(flops=4 * 10**9, bytes_accessed=10**7, transcendentals=0),
        name="join_first",
    )(me, groups, inner, *got_first)
    codes, scales = pl.pallas_call(
        join_last_kernel,
        in_specs=[in_smem()] * 4 + [anywhere()] * (peers + 1) + [in_hbm()] * 2,
        out_specs=[in_hbm(), in_hbm()],
        out_shape=results,
        input_output_aliases={peers + 5: 0, peers + 6: 1},
        scratch_shapes=[
            pltpu.VMEM((serve_n, SECOND + THIRD + 2, BLOCK, LANES), BF16),
            *buffers,
            pltpu.SemaphoreType.DMA((peers + 1,)),
            pltpu.SemaphoreType.DMA((ring,)),
            pltpu.SemaphoreType.DMA((ring,)),
        ],
        compiler_params=pltpu.CompilerParams(vmem_limit_bytes=16 * MIB),
        cost_estimate=pl.CostEstimate(flops=10**9, bytes_accessed=10**7, transcendentals=0),
        name="join_last",
    )(me, slot_of, used, end, *got_second, got_third, codes, scales)
    return (
        codes.reshape(layers, 1, 1, per_layer, BLOCK, width),
        scales.reshape(layers, 1, 1, per_layer, width),
    )


def solution(mesh):
    finer = Mesh(mesh.devices.reshape(mesh.shape["train"], *SIDES), ("train", *SERVE))

    return jax.shard_map(
        shards,
        mesh=finer,
        in_specs=(P(None, "train", SERVE), P(), P(None, "train", None)),
        out_specs=(P(None, SERVE, "train", None, None, None), P(None, SERVE, "train", None, None)),
        check_vma=False,
    )
```

```python
import functools

import jax
import jax.numpy as jnp
from jax import lax
from jax.experimental import pallas as pl
from jax.experimental.pallas import tpu as pltpu
from jax.sharding import Mesh
from jax.sharding import PartitionSpec as P


BLOCK = 32
SHIFT = 32
LANES = 128
PACK = 16
SERVE = ("x", "y", "core")
SIDES = (2, 4, 2)
OFFSETS = [
    (dx, dy, dc)
    for dx, dy, dc in (
        *((1, 2, 1), (1, 2, 0), (1, 1, 1), (0, 3, 1), (0, 1, 1), (1, 1, 0), (0, 1, 0), (0, 3, 0)),
        *((1, 3, 1), (0, 2, 1), (0, 2, 0), (1, 3, 0), (1, 0, 1), (1, 0, 0), (0, 0, 1), (0, 0, 0)),
    )
]
OPENING = 4
FIRST, SECOND, THIRD = 31, 9, 23
ENTRIES = 64
NT = (((1,), (1,)), ((), ()))
F32 = jnp.float32
BF16 = jnp.bfloat16
MIB = 1024 * 1024


def iota(shape, dim):
    return lax.broadcasted_iota(jnp.int32, shape, dim)


def identity(n):
    return (iota((n, n), 0) == iota((n, n), 1)).astype(BF16)


def layer_major():
    out, src = iota((PACK * PACK, PACK * PACK), 0), iota((PACK * PACK, PACK * PACK), 1)
    return ((out // PACK == src % PACK) & (out % PACK == src // PACK)).astype(BF16)


def rest_major():
    out, src = iota((LANES, 4 * PACK), 0), iota((LANES, 4 * PACK), 1)
    return ((out // 4 == src % PACK) & (out % 4 == src // PACK)).astype(BF16)


def dot(a, b):
    return jnp.dot(a, b, preferred_element_type=F32)


def turn(eye, value):
    return lax.dot_general(eye, value, NT, preferred_element_type=F32)


def ahead(me, offset):
    dx, dy, dc = offset
    return (me ^ (8 * dx + dc)) & 9 | ((me >> 1) + dy & 3) << 1


def behind(me, offset):
    dx, dy, dc = offset
    return ahead(me, (dx, -dy & 3, dc))


def fill(refs, me, group, start, size, end, block, ref):
    table_ref, extra_ref = refs
    lane_group = iota((BLOCK, LANES), 1) >> 2
    rest = jnp.zeros((BLOCK, LANES), F32)
    for n in range(size):
        j = start + n
        entry = jnp.where(j < end, table_ref[group * ENTRIES + j], SHIFT)
        layer, at = entry >> 10, pl.multiple_of(entry & 1023, BLOCK)
        ref[n] = block(layer, at)
        place = j + me & 31
        moved = pltpu.roll(extra_ref[pl.ds(at, BLOCK), :], 4 * (place - layer) & (LANES - 1), 1)
        rest = jnp.where(lane_group == place, moved, rest)
    ref[size] = rest.astype(BF16)


def turn_kernel(me_ref, group_hbm, x_hbm, *refs):
    set_hbm, refs = refs[:OPENING], refs[OPENING:]
    rows_hbm, extra_ref, head_ref, tail_ref, table_ref, inner_ref, end_ref, most_ref = refs[:8]
    x_ref, planes, rows_ref, first_set, group_ref, sems, out_sem, set_sem, group_sem = refs[8:]
    load = pltpu.make_async_copy(group_hbm, group_ref, group_sem)
    load.start()
    length = x_ref.shape[2]
    steps = LANES // PACK
    spare = PACK - 4
    parts = [(LANES - spare, spare, 0)] + [(PACK * i, PACK, spare + PACK * i) for i in range(steps)]
    parts.append((LANES, 4, spare + LANES))
    copies = [
        pltpu.make_async_copy(x_hbm.at[pl.ds(src, n)], x_ref.at[pl.ds(dst, n)], sems.at[i])
        for i, (src, n, dst) in enumerate(parts)
    ]
    for copy in copies:
        copy.start()
    layers, _, blocks = group_ref.shape
    groups = inner_ref.shape[0]

    def enter(count_ref, layer, b):
        group = group_ref[layer, 0, b]
        j = count_ref[group]
        count_ref[group] = j + 1
        table_ref[group * ENTRIES + j] = (layer << 10) + SHIFT + BLOCK * b

    for g in range(groups):
        inner_ref[g] = 0
    perm = layer_major()
    me = me_ref[0]
    turns, part = me >> 2, 4 * (me & 3)
    load.wait()
    copies[0].wait()
    for i in range(steps):
        copies[i + 1].wait()
        x = x_ref[pl.ds(spare + PACK * i - part, PACK)].reshape(PACK * PACK, length)
        at = pl.multiple_of(PACK * ((i + turns) & (steps - 1)), PACK)
        planes[:, pl.ds(at, PACK), :] = dot(perm, x).astype(BF16).reshape(PACK, PACK, length)
        for layer in range(layers * i // steps, layers * (i + 1) // steps):
            for b in range(1, blocks - 1):
                enter(inner_ref, layer, b)
    copies[steps + 1].wait()
    rest = dot(rest_major(), x_ref[pl.ds(spare + LANES, 4)].reshape(4 * PACK, length)).astype(BF16)
    for start in range(0, length, 256):
        size = min(256, length - start)
        extra_ref[start : start + size, :] = turn(identity(size), rest[:, start : start + size])
    for g in range(groups):
        end_ref[g] = jnp.maximum(inner_ref[g], FIRST)
    for layer in range(layers):
        for b in (0, blocks - 1):
            enter(end_ref, layer, b)
    most_ref[0] = functools.reduce(jnp.maximum, [end_ref[g] for g in range(groups)])

    def layer_step(layer, carry):
        turned = jnp.transpose(planes[layer])
        rows_ref[layer] = turned
        head_ref[layer] = turned[:SHIFT]
        tail_ref[layer] = turned[length - SHIFT :]
        pltpu.make_async_copy(rows_ref.at[layer], rows_hbm.at[layer], out_sem).start()
        return carry

    lax.fori_loop(0, layers, layer_step, 0)
    head_ref[layers] = extra_ref[:SHIFT].astype(BF16)
    tail_ref[layers] = extra_ref[length - SHIFT :].astype(BF16)
    fill_first(OFFSETS[:OPENING], me, table_ref, inner_ref, extra_ref, rows_ref, first_set, set_hbm, set_sem)
    pltpu.make_async_copy(rows_ref, rows_hbm, out_sem).wait()


def fill_first(offsets, me, table_ref, inner_ref, extra_ref, rows_ref, first_set, set_hbm, set_sem):
    stores = []
    for p, offset in enumerate(offsets):
        group = ahead(me, offset)
        fill(
            (table_ref, extra_ref), me, group, 0, FIRST, inner_ref[group],
            lambda layer, at: rows_ref[layer, pl.ds(at, BLOCK), :], first_set.at[p],
        )
        stores.append(pltpu.make_async_copy(first_set.at[p], set_hbm[p], set_sem.at[p]))
        stores[-1].start()
    for store in stores:
        store.wait()


def first_kernel(me_ref, table_ref, inner_ref, rows_hbm, extra_ref, *refs):
    offsets = OFFSETS[OPENING:]
    set_hbm, (rows_ref, first_set, sem, set_sem) = refs[: len(offsets)], refs[len(offsets) :]
    load = pltpu.make_async_copy(rows_hbm, rows_ref, sem)
    load.start()
    load.wait()
    fill_first(offsets, me_ref[0], table_ref, inner_ref, extra_ref, rows_ref, first_set, set_hbm, set_sem)


def rest_kernel(me_ref, shard_ref, offset_ref, table_ref, end_ref, rows_hbm, rest_ref, left_ref, right_ref, *refs):
    peers = len(OFFSETS)
    second_hbm, third_hbm, rows_ref, edge_ref, extra_ref, second_ref, third_ref, sems, set_sem = refs
    layers, length = rows_hbm.shape[:2]
    row = iota((BLOCK, LANES), 0)
    lane_group = iota((BLOCK, LANES), 1) >> 2
    me, shard = me_ref[0], shard_ref[0]
    last = length - 2 * SHIFT
    before = shard * (length - 2 * SHIFT)
    cuts = (pl.ds(SHIFT, SHIFT), pl.ds(last, SHIFT), pl.ds(2 * SHIFT, last - 2 * SHIFT))
    loads = [pltpu.make_async_copy(rows_hbm.at[:, cut], rows_ref.at[:, cut], sems.at[i]) for i, cut in enumerate(cuts)]
    for load in loads:
        load.start()
    for load in loads[:2]:
        load.wait()

    def edge_step(layer, carry):
        first, after = carry
        start = offset_ref[layer, shard] - before
        end = offset_ref[layer, shard + 1] - before - (last - SHIFT)
        edge_ref[layer, :SHIFT] = jnp.where(row < start, left_ref[layer], rows_ref[layer, SHIFT : 2 * SHIFT])
        edge_ref[layer, SHIFT:] = jnp.where(row >= end, right_ref[layer], rows_ref[layer, last : last + SHIFT])
        return jnp.where(lane_group == layer, start, first), jnp.where(lane_group == layer, end, after)

    nothing = jnp.zeros((BLOCK, LANES), jnp.int32)
    first, after = lax.fori_loop(0, layers, edge_step, (nothing, nothing), unroll=4)
    extra_ref[...] = rest_ref[...]
    extra_ref[SHIFT : 2 * SHIFT] = jnp.where(row < first, left_ref[layers].astype(F32), rest_ref[SHIFT : 2 * SHIFT])
    extra_ref[last : last + SHIFT] = jnp.where(row >= after, right_ref[layers].astype(F32), rest_ref[last : last + SHIFT])

    def block(layer, at):
        low, high = at == SHIFT, at == last
        edge = edge_ref[layer, pl.ds(pl.multiple_of(jnp.where(high, SHIFT, 0), BLOCK), BLOCK), :]
        return jnp.where(low | high, edge, rows_ref[layer, pl.ds(at, BLOCK), :])

    loads[2].wait()
    stores = []
    for group in range(peers):
        fill((table_ref, extra_ref), me, group, FIRST, SECOND, end_ref[group], block, second_ref.at[group])
        stores.append(pltpu.make_async_copy(second_ref.at[group], second_hbm.at[group], set_sem.at[group]))
        stores[-1].start()
    for store in stores:
        store.wait()

    def third_step(group, carry):
        @pl.when(end_ref[group] > FIRST + SECOND)
        def _():
            fill((table_ref, extra_ref), me, group, FIRST + SECOND, THIRD, end_ref[group], block, third_ref)
            store = pltpu.make_async_copy(third_ref, third_hbm.at[group], sems.at[3])
            store.start()
            store.wait()

        return carry

    lax.fori_loop(0, peers, third_step, 0)


def join_slot(held, n, tile, jj, code_ref, scale_ref, width):
    peers = held.shape[0]
    lane = iota((BLOCK, LANES), 1)
    source = (lane >> 2) - jj & 31
    rest = jnp.zeros((BLOCK, LANES), F32)
    for s in range(peers):
        rest = jnp.where(source == s, held[s, tile].astype(F32), rest)
    rest = pltpu.roll(rest, -4 * jj & (LANES - 1), 1)
    before = None
    for t in range(peers + 1):
        x = rest
        if before is not None:
            x = jnp.where(lane < 4 * t - 4, before, x)
        if t < peers:
            own = held[t, n].astype(F32)
            x = own if t == 0 else jnp.where(lane >= 4 * t, own, x)
            before = own
        size = min(LANES, width - LANES * t)
        top = jnp.maximum(jnp.max(jnp.abs(x), axis=0, keepdims=True), 0.25)
        scale_ref[:, LANES * t : LANES * t + size] = top[:, :size]
        code_ref[:, LANES * t : LANES * t + size] = (x * (1.0 / top)).astype(BF16)[:, :size]


def write_slots(codes_hbm, scale_hbm, code_ref, scale_ref, code_sem, scale_sem, low, high, slot_of, compute):
    ring = code_ref.shape[0]

    def stores(i, slot):
        return (
            pltpu.make_async_copy(code_ref.at[i], codes_hbm.at[slot], code_sem.at[i]),
            pltpu.make_async_copy(scale_ref.at[i], scale_hbm.at[slot], scale_sem.at[i]),
        )

    def step(j, carry):
        i = j - low & (ring - 1)

        @pl.when(j - low >= ring)
        def _():
            for store in stores(i, 0):
                store.wait()

        compute(j, code_ref.at[i], scale_ref.at[i])
        for store in stores(i, slot_of(j)):
            store.start()
        return carry

    lax.fori_loop(low, high, step, 0)
    for i in range(ring):

        @pl.when(high - low > i)
        def _(i=i):
            for store in stores(i, 0):
                store.wait()


def join_first_kernel(me_ref, group_hbm, inner_ref, *refs):
    peers = len(OFFSETS)
    parts, (codes_hbm, scale_hbm, late_ref) = refs[:peers], refs[peers : peers + 3]
    held, code_ref, scale_ref, zero_code, zero_scale, group_ref, slot_ref, used_ref = refs[peers + 3 : peers + 11]
    sems, code_sem, scale_sem, zero_sem = refs[peers + 11 :]
    me, width = me_ref[0], codes_hbm.shape[2]
    layers, _, blocks = group_ref.shape
    load = pltpu.make_async_copy(group_hbm, group_ref, sems.at[peers])
    load.start()
    load.wait()
    per_layer = codes_hbm.shape[0] // layers
    loads = [pltpu.make_async_copy(part, held.at[behind(me, o)], sems.at[p]) for p, (part, o) in enumerate(zip(parts, OFFSETS))]
    for load in loads:
        load.start()
    zero_code[...] = jnp.zeros_like(zero_code)
    zero_scale[...] = jnp.zeros_like(zero_scale)

    unused = ENTRIES

    def find(layer, carry):
        inner, edge = carry
        k = jnp.int32(0)
        for b in range(blocks):
            mine = (group_ref[layer, 0, b] == me).astype(jnp.int32)
            at_edge = b in (0, blocks - 1)
            slot_ref[jnp.where(mine == 1, edge if at_edge else inner, unused)] = per_layer * layer + k
            k = k + mine
            inner, edge = (inner, edge + mine) if at_edge else (inner + mine, edge)
        used_ref[layer] = k
        return inner, edge

    inner, edge = lax.fori_loop(0, layers, find, (jnp.int32(0), jnp.maximum(inner_ref[me], FIRST)))
    for j in range(FIRST, ENTRIES):
        late_ref[j - FIRST] = slot_ref[j]
    late_ref[ENTRIES - FIRST] = edge
    late_ref[ENTRIES - FIRST + 1] = me

    def clear(slot):
        return (
            pltpu.make_async_copy(zero_code, codes_hbm.at[slot], zero_sem.at[0]),
            pltpu.make_async_copy(zero_scale, scale_hbm.at[slot], zero_sem.at[1]),
        )

    def each_empty(act):
        def layer_step(layer, carry):
            for k in range(per_layer):

                @pl.when(k >= used_ref[layer])
                def _(k=k):
                    for copy in clear(per_layer * layer + k):
                        act(copy)

            return carry

        lax.fori_loop(0, layers, layer_step, 0)

    each_empty(lambda copy: copy.start())
    for load in loads:
        load.wait()

    def compute(j, code, scale):
        join_slot(held, j, FIRST, j, code, scale, width)

    write_slots(
        codes_hbm, scale_hbm, code_ref, scale_ref, code_sem, scale_sem,
        0, jnp.minimum(inner, FIRST), lambda j: slot_ref[j], compute,
    )
    each_empty(lambda copy: copy.wait())


def join_last_kernel(late_ref, second_hbm, third_hbm, *refs):
    codes_hbm, scale_hbm, held, code_ref, scale_ref, sems, code_sem, scale_sem = refs[2:]
    end, width = late_ref[ENTRIES - FIRST], codes_hbm.shape[2]
    second = pltpu.make_async_copy(second_hbm, held.at[:, pl.ds(0, SECOND + 1)], sems.at[0])
    second.start()

    @pl.when(end > FIRST + SECOND)
    def _():
        load = pltpu.make_async_copy(third_hbm, held.at[:, pl.ds(SECOND + 1, THIRD + 1)], sems.at[1])
        load.start()
        load.wait()

    second.wait()

    def compute(j, code, scale):
        late = (j >= FIRST + SECOND).astype(jnp.int32)
        join_slot(held, j - FIRST + late, SECOND + late * (THIRD + 1), j & 31, code, scale, width)

    write_slots(
        codes_hbm, scale_hbm, code_ref, scale_ref, code_sem, scale_sem,
        FIRST, end, lambda j: late_ref[j - FIRST], compute,
    )


def in_vmem():
    return pl.BlockSpec(memory_space=pltpu.VMEM)


def in_hbm():
    return pl.BlockSpec(memory_space=pltpu.HBM)


def anywhere():
    return pl.BlockSpec(memory_space=pl.ANY)


def hbm(value):
    return pltpu.with_memory_space_constraint(value, pltpu.HBM)


def in_smem():
    return pl.BlockSpec(memory_space=pltpu.SMEM)


def sent_to(value, offset):
    count = SIDES[0] * SIDES[1] * SIDES[2]
    return lax.ppermute(value, SERVE, [(i, ahead(i, offset)) for i in range(count)])


def shards(train_weights, row_offset, block_group):
    train_n = lax.axis_size("train")
    serve_n = lax.axis_size(SERVE)
    train_idx = lax.axis_index("train")
    serve_idx = lax.axis_index(SERVE).astype(jnp.int32)
    layers, buffer_len, columns = train_weights.shape
    blocks_dev = block_group.shape[1]
    per_layer = (blocks_dev + serve_n - 1) // serve_n + 1
    slots = layers * per_layer
    width = columns * serve_n
    groups = hbm(jnp.transpose(block_group, (0, 2, 1)))
    me, shard = serve_idx.reshape(1), train_idx.astype(jnp.int32).reshape(1)
    by_column = hbm(jnp.transpose(train_weights, (2, 0, 1)))

    peers = len(OFFSETS)
    steps = LANES // PACK
    edge = jax.ShapeDtypeStruct((layers + 1, SHIFT, LANES), BF16)
    per_group = jax.ShapeDtypeStruct((serve_n,), jnp.int32)
    turned = pl.pallas_call(
        turn_kernel,
        in_specs=[in_smem(), in_hbm(), in_hbm()],
        out_specs=[in_hbm()] * (OPENING + 1) + [in_vmem()] * 3 + [in_smem()] * 4,
        out_shape=[pltpu.HBM((FIRST + 1, BLOCK, LANES), BF16)] * OPENING
        + [
            pltpu.HBM((layers, buffer_len, LANES), BF16),
            jax.ShapeDtypeStruct((buffer_len, LANES), F32),
            edge,
            edge,
            jax.ShapeDtypeStruct((serve_n * ENTRIES,), jnp.int32),
            per_group,
            per_group,
            jax.ShapeDtypeStruct((1,), jnp.int32),
        ],
        scratch_shapes=[
            pltpu.VMEM((columns + PACK - 4, layers, buffer_len), BF16),
            pltpu.VMEM((layers, LANES, buffer_len), BF16),
            pltpu.VMEM((layers, buffer_len, LANES), BF16),
            pltpu.VMEM((OPENING, FIRST + 1, BLOCK, LANES), BF16),
            pltpu.SMEM((layers, 1, blocks_dev), jnp.int32),
            pltpu.SemaphoreType.DMA((steps + 2,)),
            pltpu.SemaphoreType.DMA,
            pltpu.SemaphoreType.DMA((OPENING,)),
            pltpu.SemaphoreType.DMA,
        ],
        compiler_params=pltpu.CompilerParams(vmem_limit_bytes=24 * MIB),
        cost_estimate=pl.CostEstimate(flops=3 * 10**9, bytes_accessed=9 * 10**6, transcendentals=0),
        name="turn",
    )(me, groups, by_column)
    rows, rest, head, tail, table, inner, end, most = turned[OPENING:]
    others = peers - OPENING
    first_sent = turned[:OPENING] + pl.pallas_call(
        first_kernel,
        in_specs=[in_smem()] * 3 + [in_hbm(), in_vmem()],
        out_specs=[in_hbm()] * others,
        out_shape=[pltpu.HBM((FIRST + 1, BLOCK, LANES), BF16)] * others,
        scratch_shapes=[
            pltpu.VMEM((layers, buffer_len, LANES), BF16),
            pltpu.VMEM((others, FIRST + 1, BLOCK, LANES), BF16),
            pltpu.SemaphoreType.DMA,
            pltpu.SemaphoreType.DMA((others,)),
        ],
        compiler_params=pltpu.CompilerParams(vmem_limit_bytes=16 * MIB),
        cost_estimate=pl.CostEstimate(flops=10**9, bytes_accessed=10**7, transcendentals=0),
        name="first_set",
    )(me, table, inner, hbm(rows), rest)
    left = lax.ppermute(tail, "train", [(i, i + 1) for i in range(train_n - 1)])
    right = lax.ppermute(head, "train", [(i + 1, i) for i in range(train_n - 1)])
    second_sent, third_sent = pl.pallas_call(
        rest_kernel,
        in_specs=[in_smem()] * 5 + [in_hbm()] + [in_vmem()] * 3,
        out_specs=[in_hbm(), in_hbm()],
        out_shape=[pltpu.HBM((serve_n, n + 1, BLOCK, LANES), BF16) for n in (SECOND, THIRD)],
        scratch_shapes=[
            pltpu.VMEM((layers, buffer_len, LANES), BF16),
            pltpu.VMEM((layers, 2 * SHIFT, LANES), BF16),
            pltpu.VMEM((buffer_len, LANES), F32),
            pltpu.VMEM((serve_n, SECOND + 1, BLOCK, LANES), BF16),
            pltpu.VMEM((THIRD + 1, BLOCK, LANES), BF16),
            pltpu.SemaphoreType.DMA((4,)),
            pltpu.SemaphoreType.DMA((serve_n,)),
        ],
        compiler_params=pltpu.CompilerParams(vmem_limit_bytes=16 * MIB),
        cost_estimate=pl.CostEstimate(flops=10**9, bytes_accessed=10**7, transcendentals=0),
        name="rest",
    )(me, shard, row_offset, table, end, hbm(rows), rest, left, right)

    got_first = [sent_to(v, o) for v, o in zip(first_sent[:OPENING], OFFSETS)]
    got_first += [sent_to(v, o) for v, o in zip(first_sent[OPENING:-1], OFFSETS[OPENING:])] + [first_sent[-1]]
    got_second = lax.all_to_all(second_sent, SERVE, split_axis=0, concat_axis=0, tiled=True)
    got_third = lax.cond(
        most.reshape(()) > FIRST + SECOND,
        lambda v: lax.all_to_all(v, SERVE, split_axis=0, concat_axis=0, tiled=True),
        lambda v: v,
        third_sent,
    )
    ring = 8
    results = [pltpu.HBM((slots, BLOCK, width), BF16), pltpu.HBM((slots, 1, width), F32)]
    buffers = [pltpu.VMEM((ring, BLOCK, width), BF16), pltpu.VMEM((ring, 1, width), F32)]
    codes, scales, late = pl.pallas_call(
        join_first_kernel,
        in_specs=[in_smem(), in_hbm(), in_smem()] + [in_hbm()] * (peers - 1) + [anywhere()],
        out_specs=[in_hbm(), in_hbm(), in_smem()],
        out_shape=results + [jax.ShapeDtypeStruct((ENTRIES - FIRST + 2,), jnp.int32)],
        scratch_shapes=[
            pltpu.VMEM((serve_n, FIRST + 1, BLOCK, LANES), BF16),
            *buffers,
            pltpu.VMEM((BLOCK, width), BF16),
            pltpu.VMEM((1, width), F32),
            pltpu.SMEM((layers, 1, blocks_dev), jnp.int32),
            pltpu.SMEM((ENTRIES + 1,), jnp.int32),
            pltpu.SMEM((layers,), jnp.int32),
            pltpu.SemaphoreType.DMA((peers + 1,)),
            pltpu.SemaphoreType.DMA((ring,)),
            pltpu.SemaphoreType.DMA((ring,)),
            pltpu.SemaphoreType.DMA((2,)),
        ],
        compiler_params=pltpu.CompilerParams(vmem_limit_bytes=16 * MIB),
        cost_estimate=pl.CostEstimate(flops=4 * 10**9, bytes_accessed=10**7, transcendentals=0),
        name="join_first",
    )(me, groups, inner, *map(hbm, got_first[:-1]), got_first[-1])
    codes, scales = pl.pallas_call(
        join_last_kernel,
        in_specs=[in_smem(), anywhere()] + [in_hbm()] * 3,
        out_specs=[in_hbm(), in_hbm()],
        out_shape=results,
        input_output_aliases={3: 0, 4: 1},
        scratch_shapes=[
            pltpu.VMEM((serve_n, SECOND + THIRD + 2, BLOCK, LANES), BF16),
            *buffers,
            pltpu.SemaphoreType.DMA((2,)),
            pltpu.SemaphoreType.DMA((ring,)),
            pltpu.SemaphoreType.DMA((ring,)),
        ],
        compiler_params=pltpu.CompilerParams(vmem_limit_bytes=16 * MIB),
        cost_estimate=pl.CostEstimate(flops=10**9, bytes_accessed=10**7, transcendentals=0),
        name="join_last",
    )(late, got_second, hbm(got_third), codes, scales)
    return (
        codes.reshape(layers, 1, 1, per_layer, BLOCK, width),
        scales.reshape(layers, 1, 1, per_layer, width),
    )


def solution(mesh):
    finer = Mesh(mesh.devices.reshape(mesh.shape["train"], *SIDES), ("train", *SERVE))

    return jax.shard_map(
        shards,
        mesh=finer,
        in_specs=(P(None, "train", SERVE), P(), P(None, "train", None)),
        out_specs=(P(None, SERVE, "train", None, None, None), P(None, SERVE, "train", None, None)),
        check_vma=False,
    )
```
